768 devices in a mesh: gx: 64 (over y, x, core), gy: 12 (over z).
Axes of the slice: x: 4, y: 8, z: 12, core: 2. Of those that a mesh axis runs over, the one named last changes fastest.
Arguments:
- right_side: float32 [1024, 768, 192], P('gx', 'gy'), may hold values from -46 to 46
- diagonal: float32 [1024, 768, 192], P('gx', 'gy'), may hold values from 0.1 to 2
Outputs:
- solution_field: float32 [1024, 768, 192], P('gx', 'gy')
- residual: float32 [1024, 768, 192], P('gx', 'gy')
The draws below stay inside these ranges and needn't reach their ends.
All inputs are finite; a program needn't handle non-finite values.
Results may differ from the reference program's by a relative error of at most 0.00017.
Values sent between devices are 32-bit elements; how exact they have to be, the bound alone decides.
No kernel may reach another device: no remote copies, remote signals or barrier semaphores. Data moves between devices by JAX's collectives and lax.ppermute only.
A program may use at most 32 MiB of HBM per device.

```python
import math
import jax
import jax.numpy as jnp

CZ = 192
ITERS = 3
NX = 1024
NY = 768


def draw_right_side(key, part):
    first = jax.random.fold_in(key, 11)
    second = jax.random.fold_in(key, 12)
    ramp = 1.0 + 2.0 * jnp.arange(NX, dtype=jnp.float32) / max(NX - 1, 1)
    ramp = ramp.reshape(NX, 1, 1)
    base = jnp.clip(jax.random.normal(first, (NX, NY, CZ), jnp.float32), -5.0, 5.0)
    column = jnp.exp(jax.random.uniform(second, (NX, NY, 1), jnp.float32) * math.log(3.0))
    return ramp * column * base


def levels(rng, extent, split, least, high):
    gain = 1.0
    for position, parts in split:
        draws = jax.random.uniform(jax.random.fold_in(jax.random.fold_in(rng, 6), position), (parts,), jnp.float32, least / len(split), high / len(split))
        gain = gain * jnp.repeat(jnp.exp(draws), extent[position] // parts).reshape((-1,) + (1,) * (len(extent) - 1 - position))
    return gain


def setup_inputs(seed: int = 0) -> dict:
    arg_keys = jax.random.split(jax.random.key(seed), 3)
    return {
        "right_side": draw_right_side(jax.random.fold_in(arg_keys[2], 71), 0),
        "diagonal": jnp.clip(jnp.exp(math.log(2.0) - 2.9957323 * jax.random.uniform(arg_keys[1], (NX, NY, CZ), jnp.float32) ** levels(arg_keys[1], (NX, NY, CZ), ((0, 64), (1, 12)), -0.2, 0.2)), 0.1, 2.0),
    }


def operate(field, diagonal):
    padded = jnp.pad(field, 1)
    beside = padded[2:, 1:-1, 1:-1] + padded[:-2, 1:-1, 1:-1]
    beside = beside + padded[1:-1, 2:, 1:-1] + padded[1:-1, :-2, 1:-1]
    beside = beside + padded[1:-1, 1:-1, 2:] + padded[1:-1, 1:-1, :-2]
    return (6.0 + diagonal) * field - beside


def reference(right_side, diagonal):
    solution_field = jnp.zeros_like(right_side)
    residual = right_side
    w_field = operate(right_side, diagonal)
    z_field = jnp.zeros_like(right_side)
    s_field = jnp.zeros_like(right_side)
    p_field = jnp.zeros_like(right_side)
    gamma_prev = jnp.float32(1.0)
    alpha_prev = jnp.float32(1.0)
    for step in range(ITERS):
        gamma = jnp.sum(residual * residual)
        delta = jnp.sum(w_field * residual)
        if step == 0:
            beta = jnp.float32(0.0)
            alpha = gamma / delta
        else:
            beta = gamma / gamma_prev
            alpha = gamma / (delta - beta * gamma / alpha_prev)
        s_field = w_field + beta * s_field
        p_field = residual + beta * p_field
        solution_field = solution_field + alpha * p_field
        residual = residual - alpha * s_field
        if step + 1 < ITERS:
            q_field = operate(w_field, diagonal)
            z_field = q_field + beta * z_field
            w_field = w_field - alpha * z_field
        gamma_prev = gamma
        alpha_prev = alpha
    return solution_field, residual
```

```python
import jax
import jax.numpy as jnp
from jax import lax
from jax.experimental import pallas as pl
from jax.experimental.pallas import tpu as pltpu
from jax.sharding import Mesh
from jax.sharding import PartitionSpec as P


SHIFT = 7.0
GRAIN = 8.0
GX = ("y", "x", "c")
FIRST = ("y", "c")
SECOND = ("x", "z")
F32 = jnp.float32
DEPTH = 3


def two_sum(a, b):
    s = a + b
    t = s - a
    return s, (a - (s - t)) + (b - t)


def halves(a):
    t = a * 4097.0
    high = t - (t - a)
    return high, a - high


def scaled(pair, factor):
    high, low = halves(pair[0])
    s, e = two_sum(high * factor, low * factor)
    return s, e + pair[1] * factor


def added(one, two):
    s, e = two_sum(one[0], two[0])
    return two_sum(s, e + (one[1] + two[1]))


def translated(moments, step):
    row = list(moments)
    out = [row[0]]
    while len(row) > 1:
        row = [added(row[k + 1], scaled(row[k], step)) for k in range(len(row) - 1)]
        out.append(row[0])
    return out


def to_grain(x):
    return jnp.floor(x * GRAIN + 0.5) / GRAIN


def iota(shape, dim):
    return lax.broadcasted_iota(jnp.int32, shape, dim)


def pack_y(b, d, forward, backward):
    nx, ny, nz = b.shape
    sub = iota((nx, 8, nz), 1)
    last = d[:, ny - 8 : ny, :]
    forward[...] = jnp.where(sub >= 5, b[:, ny - 8 : ny, :], pltpu.roll(last, 4, 1))
    backward[...] = jnp.where(sub < 3, b[:, 0:8, :], pltpu.roll(d[:, 0:8, :], 4, 1))


def rims(low, high):
    sub = iota(low.shape, low.ndim - 2)
    field = jnp.where(sub >= 5, low, jnp.where(sub < 3, high, 0.0))
    low_shift = pltpu.roll(low, 4, low.ndim - 2)
    high_shift = pltpu.roll(high, 4, low.ndim - 2)
    shift = jnp.where(sub >= 6, low_shift, jnp.where(sub < 2, high_shift, 0.0))
    return field, shift


def pack_x(b, d, ylow, yhigh, forward, backward):
    nx, ny, nz = b.shape
    for out, bx, dx in ((forward, nx - 3, nx - 2), (backward, 0, 0)):
        out[0:3, 0:ny, :] = b[bx : bx + 3, :, :]
        out[3:5, 0:ny, :] = d[dx : dx + 2, :, :]
        field, _ = rims(ylow[bx : bx + 3], yhigh[bx : bx + 3])
        _, shift = rims(ylow[dx : dx + 2], yhigh[dx : dx + 2])
        out[0:3, ny : ny + 8, :] = field
        out[3:5, ny : ny + 8, :] = shift


def wide(a):
    nz = a.shape[-1]
    return jnp.pad(a, ((0, 0),) * (a.ndim - 1) + ((0, 256 - nz),))


def fields(edge, b, d, ylow, yhigh, xlow, xhigh, u1, u2, u3, row_out, c_out, u0, dx, keep):
    nx, ny, nz = b.shape
    rows = ny + 16

    def place(into, at, own, rim):
        sub = iota((8, 256), 0)
        rim = wide(rim)
        into[at, 8 : 8 + ny, :] = wide(own)
        into[at, 0:8, :] = jnp.where(sub >= 5, rim, 0.0)
        into[at, 8 + ny : rows, :] = jnp.where(sub < 3, rim, 0.0)

    def own(i, carry):
        field, shift = rims(ylow[i], yhigh[i])
        place(u0, i + 3, b[i], field)
        place(dx, i + 2, d[i], shift)
        return carry

    lax.fori_loop(0, nx, own, 0)
    for j in range(3):
        place(u0, j, xlow[j, 0:ny], xlow[j, ny : ny + 8])
        place(u0, nx + 3 + j, xhigh[j, 0:ny], xhigh[j, ny : ny + 8])
    for j in range(2):
        place(dx, j, xlow[3 + j, 0:ny], xlow[3 + j, ny : ny + 8])
        place(dx, nx + 2 + j, xhigh[3 + j, 0:ny], xhigh[3 + j, ny : ny + 8])
    at_row = iota((rows, 256), 0)
    side = jnp.where(at_row < 8, edge[2], jnp.where(at_row >= 8 + ny, edge[3], 1.0))
    keep[...] = jnp.where(iota((rows, 256), 1) < nz, side, 0.0)

    def applied(field, at, shift_at, base):
        mid = field[at]
        beside = field[at - 1] + field[at + 1]
        beside = beside + (pltpu.roll(mid, 1, 0) + pltpu.roll(mid, rows - 1, 0))
        beside = beside + (pltpu.roll(mid, 1, 1) + pltpu.roll(mid, 255, 1))
        return (dx[shift_at] + base) * mid - beside

    def folded(a):
        return jnp.sum(a[8 : 8 + ny].reshape(ny // 8, 8, 256), axis=0)

    def total(a):
        return jnp.sum(a, axis=(0, 1), keepdims=True)

    def probe(i, carry):
        mid = u0[4 * i + 3] * keep[...]
        return carry[0] + folded(mid * mid), carry[1] + folded(mid * applied(u0, 4 * i + 3, 4 * i + 2, 6.0))

    zero = jnp.zeros((8, 256), F32)
    norm, lift = lax.fori_loop(0, nx // 4, probe, (zero, zero))
    norm = total(norm)
    lift = total(lift)
    shift = jnp.where(norm > 0.0, lift / jnp.where(norm > 0.0, norm, 1.0), SHIFT)
    shift = to_grain(jnp.clip(shift, 0.0, 14.0))
    base = 6.0 - shift

    def along(i, count):
        return jnp.where(i < count, edge[0], jnp.where(i >= nx + count, edge[1], 1.0))

    def first(i, carry):
        u1[i] = applied(u0, i + 1, i, base) * (keep[...] * along(i, 2))
        return carry

    def second(i, carry):
        u2[i] = applied(u1, i + 1, i + 1, base) * (keep[...] * along(i, 1))
        return carry

    def third(i, carry):
        new = applied(u2, i + 1, i + 2, base) * keep[...]
        u3[i] = new[8 : 8 + ny]
        f0 = u0[i + 3]
        f1 = u1[i + 2]
        f2 = u2[i + 1]
        return (
            carry[0] + folded(f0 * f0),
            carry[1] + folded(f0 * f1),
            carry[2] + folded(f1 * f1),
            carry[3] + folded(f1 * f2),
            carry[4] + folded(f2 * f2),
            carry[5] + folded(f2 * new),
        )

    lax.fori_loop(0, nx + 4, first, 0)
    lax.fori_loop(0, nx + 2, second, 0)
    sums = lax.fori_loop(0, nx, third, (zero,) * 6)
    sums = [jnp.broadcast_to(total(a), (8, 128)) for a in sums]
    step = jnp.broadcast_to(shift, (8, 128)) - SHIFT
    pairs = translated([(a, jnp.zeros((8, 128), F32)) for a in sums], step)
    lane = iota((8, 128), 1)
    line = jnp.zeros((8, 128), F32)
    for k, (high, low) in enumerate(pairs):
        line = jnp.where(lane == k, high, jnp.where(lane == k + 6, low, line))
    for k in range(row_out.shape[0] // 8):
        row_out[8 * k : 8 * k + 8, :] = line
    c_out[...] = jnp.broadcast_to(shift, (8, 128))


def gathered(rows):
    parts = [(rows[8 * k : 8 * k + 8], jnp.zeros((8, 128), F32)) for k in range(rows.shape[0] // 8)]

    def joined(one, two):
        s, e = two_sum(one[0], two[0])
        return s, e + (one[1] + two[1])

    while len(parts) > 1:
        parts = [joined(*parts[k : k + 2]) if k + 1 < len(parts) else parts[k] for k in range(0, len(parts), 2)]
    s, e = parts[0]
    for by in (4, 2, 1):
        s, e = joined((s, e), (pltpu.roll(s, by, 0), pltpu.roll(e, by, 0)))
    lane = iota((8, 128), 1)
    return jnp.where(lane < 6, s, s + pltpu.roll(e, 6, 1))


def regroup(rows, out):
    line = gathered(rows)
    for k in range(out.shape[0] // 8):
        out[8 * k : 8 * k + 8, :] = line


def steps_of(moments, centre):
    def form(one, two):
        out = 0.0
        for k in range(len(one) + len(two) - 1):
            part = 0.0
            for i in range(len(one)):
                if 0 <= k - i < len(two):
                    part = part + one[i] * two[k - i]
            out = out + part * moments[k]
        return out

    def plus(one, factor, two):
        size = max(len(one), len(two))
        out = []
        for k in range(size):
            if k >= len(two):
                out.append(one[k])
            elif k >= len(one):
                out.append(factor * two[k])
            else:
                out.append(one[k] + factor * two[k])
        return out

    unit = jnp.ones_like(moments[0])
    residual = [unit]
    solution_field = []
    s = []
    p = []
    for step in range(3):
        raised = [residual[0] * centre]
        for k in range(1, len(residual)):
            raised.append(residual[k - 1] + centre * residual[k])
        raised.append(residual[-1])
        gamma = form(residual, residual)
        delta = form(residual, raised)
        if step == 0:
            alpha = gamma / delta
            s, p = raised, residual
        else:
            beta = gamma / gamma_prev
            alpha = gamma / (delta - beta * gamma / alpha_prev)
            s = plus(raised, beta, s)
            p = plus(residual, beta, p)
        solution_field = plus(solution_field, alpha, p)
        residual = plus(residual, -alpha, s)
        gamma_prev = gamma
        alpha_prev = alpha
    return solution_field, residual


def recentred(coefficients, step):
    out = list(coefficients)
    size = len(out)
    for i in range(size - 1):
        for k in range(size - 2, i - 1, -1):
            out[k] = out[k] + step * out[k + 1]
    return out


def finish(rows, c_in, b, u1, u2, u3, solution_field, residual, coef):
    nz = b.shape[2]
    i = pl.program_id(0)
    block = b.shape[0]

    @pl.when(i == 0)
    def _():
        line = gathered(rows)
        lane = lambda k: jnp.broadcast_to(jnp.sum(jnp.where(iota((8, 128), 1) == k, line, 0.0), axis=1, keepdims=True), (8, 128))
        moments = [(lane(k), lane(k + 6)) for k in range(6)]
        away = to_grain(moments[1][0] / moments[0][0])
        moments = [high + low for high, low in translated(moments, -away)]
        centre = SHIFT + away
        xs, rs = steps_of(moments, centre)
        step = c_in[...] - centre
        xs = recentred(xs, step)
        rs = recentred(rs, step)
        for k, value in enumerate(xs + rs):
            coef[k] = value

    def coefficient(k):
        return coef[k, 0:1, 0:1]

    for j in range(block):
        at = i * block + j
        f0 = b[j]
        f1 = u1[at + 2, 8:-8, 0:nz]
        f2 = u2[at + 1, 8:-8, 0:nz]
        f3 = u3[at, :, 0:nz]
        solution_field[j] = coefficient(0) * f0 + coefficient(1) * f1 + coefficient(2) * f2
        residual[j] = coefficient(3) * f0 + coefficient(4) * f1 + coefficient(5) * f2 + coefficient(6) * f3


def shifted(a, axis, by):
    count = lax.axis_size(axis)
    pairs = [(k, k + by) for k in range(count) if 0 <= k + by < count]
    return lax.ppermute(a, axis, pairs)


def spread(rows, axes):
    count = lax.axis_size(axes)
    out = lax.all_to_all(rows[:count].reshape(count, 1, 128), axes, 0, 0, tiled=True)
    return jnp.pad(out.reshape(count, 128), ((0, -count % 8), (0, 0)))


VMEM = pl.BlockSpec(memory_space=pltpu.VMEM)
SMEM = pl.BlockSpec(memory_space=pltpu.SMEM)


def call(body, out_shapes, count, scratch=(), smem=0, name=None):
    return pl.pallas_call(
        body,
        out_shape=out_shapes,
        in_specs=[SMEM] * smem + [VMEM] * (count - smem),
        out_specs=[VMEM] * len(out_shapes),
        scratch_shapes=list(scratch),
        name=name,
    )


def on_device(right_side, diagonal):
    nx, ny, nz = right_side.shape
    rows = ny + 16
    shape = lambda *dims: jax.ShapeDtypeStruct(dims, F32)
    yf, yb = call(pack_y, (shape(nx, 8, nz),) * 2, 2, name="pack_y")(right_side, diagonal)
    ylow = shifted(yf, "z", 1)
    yhigh = shifted(yb, "z", -1)
    xf, xb = call(pack_x, (shape(5, ny + 8, nz),) * 2, 4, name="pack_x")(right_side, diagonal, ylow, yhigh)
    xlow = shifted(xf, GX, 1)
    xhigh = shifted(xb, GX, -1)
    gx = lax.axis_index(GX)
    gy = lax.axis_index("z")
    edge = jnp.stack(
        [gx > 0, gx < lax.axis_size(GX) - 1, gy > 0, gy < lax.axis_size("z") - 1]
    ).astype(F32)
    up = lambda n: -(-n // 8) * 8
    one = lax.axis_size(FIRST)
    two = lax.axis_size(SECOND)
    u1, u2, u3, line, shift = call(
        fields,
        (shape(nx + 4, rows, 256), shape(nx + 2, rows, 256), shape(nx, ny, 256), shape(up(one), 128), shape(8, 128)),
        7,
        scratch=(pltpu.VMEM((nx + 6, rows, 256), F32), pltpu.VMEM((nx + 4, rows, 256), F32), pltpu.VMEM((rows, 256), F32)),
        smem=1,
        name="fields",
    )(edge, right_side, diagonal, ylow, yhigh, xlow, xhigh)
    line = spread(line, FIRST)
    (line,) = call(regroup, (shape(up(two), 128),), 1, name="regroup")(line)
    line = spread(line, SECOND)
    block = 2
    tile = pl.BlockSpec((block, ny, nz), lambda i: (i, 0, 0))
    return pl.pallas_call(
        finish,
        out_shape=(shape(nx, ny, nz),) * 2,
        grid=(nx // block,),
        in_specs=[VMEM, VMEM, tile, VMEM, VMEM, VMEM],
        out_specs=[tile, tile],
        scratch_shapes=[pltpu.VMEM((7, 8, 128), F32)],
        name="finish",
    )(line, shift, right_side, u1, u2, u3)


def solution_on(mesh, split):
    torus = Mesh(mesh.devices.reshape(*split, mesh.shape["gy"]), GX + ("z",))
    placed = (P(GX, "z", None), P(GX, "z", None))
    return jax.shard_map(on_device, mesh=torus, in_specs=placed, out_specs=placed, check_vma=False)


def solution(mesh):
    return solution_on(mesh, (8, 4, 2))
```

```python
import jax
import jax.numpy as jnp
from jax import lax
from jax.experimental import pallas as pl
from jax.experimental.pallas import tpu as pltpu
from jax.sharding import Mesh
from jax.sharding import PartitionSpec as P


SHIFT = 7.0
GRAIN = 8.0
GX = ("y", "x", "c")
FIRST = ("y", "c")
SECOND = ("x", "z")
F32 = jnp.float32
GRANT = 24 << 20


def two_sum(a, b):
    s = a + b
    t = s - a
    return s, (a - (s - t)) + (b - t)


def halves(a):
    t = a * 4097.0
    high = t - (t - a)
    return high, a - high


def scaled(pair, factor):
    high, low = halves(pair[0])
    s, e = two_sum(high * factor, low * factor)
    return s, e + pair[1] * factor


def added(one, two):
    s, e = two_sum(one[0], two[0])
    return two_sum(s, e + (one[1] + two[1]))


def translated(moments, step):
    row = list(moments)
    out = [row[0]]
    while len(row) > 1:
        row = [added(row[k + 1], scaled(row[k], step)) for k in range(len(row) - 1)]
        out.append(row[0])
    return out


def to_grain(x):
    return jnp.floor(x * GRAIN + 0.5) / GRAIN


def iota(shape, dim):
    return lax.broadcasted_iota(jnp.int32, shape, dim)


def pack_y(b, d, forward, backward):
    nx, ny, nz = b.shape
    sub = iota((nx, 8, nz), 1)
    last = d[:, ny - 8 : ny, :]
    forward[...] = jnp.where(sub >= 5, b[:, ny - 8 : ny, :], pltpu.roll(last, 4, 1))
    backward[...] = jnp.where(sub < 3, b[:, 0:8, :], pltpu.roll(d[:, 0:8, :], 4, 1))


def rims(low, high):
    sub = iota(low.shape, low.ndim - 2)
    field = jnp.where(sub >= 5, low, jnp.where(sub < 3, high, 0.0))
    low_shift = pltpu.roll(low, 4, low.ndim - 2)
    high_shift = pltpu.roll(high, 4, low.ndim - 2)
    shift = jnp.where(sub >= 6, low_shift, jnp.where(sub < 2, high_shift, 0.0))
    return field, shift


def pack_x(b, d, ylow, yhigh, forward, backward):
    nx, ny, nz = b.shape
    for out, bx, dx in ((forward, nx - 3, nx - 2), (backward, 0, 0)):
        out[0:3, 0:ny, :] = b[bx : bx + 3, :, :]
        out[3:5, 0:ny, :] = d[dx : dx + 2, :, :]
        field, _ = rims(ylow[bx : bx + 3], yhigh[bx : bx + 3])
        _, shift = rims(ylow[dx : dx + 2], yhigh[dx : dx + 2])
        out[0:3, ny : ny + 8, :] = field
        out[3:5, ny : ny + 8, :] = shift


def wide(a):
    nz = a.shape[-1]
    return jnp.pad(a, ((0, 0),) * (a.ndim - 1) + ((0, 256 - nz),))


def fields(edge, b, d, ylow, yhigh, xlow, xhigh, u1, u2, u3, row_out, c_out, u0, dx, keep):
    nx, ny, nz = b.shape
    rows = ny + 16

    def place(into, at, own, rim):
        sub = iota((8, 256), 0)
        rim = wide(rim)
        into[at, 8 : 8 + ny, :] = wide(own)
        into[at, 0:8, :] = jnp.where(sub >= 5, rim, 0.0)
        into[at, 8 + ny : rows, :] = jnp.where(sub < 3, rim, 0.0)

    def own(i, carry):
        field, shift = rims(ylow[i], yhigh[i])
        place(u0, i + 3, b[i], field)
        place(dx, i + 2, d[i], shift)
        return carry

    lax.fori_loop(0, nx, own, 0)
    for j in range(3):
        place(u0, j, xlow[j, 0:ny], xlow[j, ny : ny + 8])
        place(u0, nx + 3 + j, xhigh[j, 0:ny], xhigh[j, ny : ny + 8])
    for j in range(2):
        place(dx, j, xlow[3 + j, 0:ny], xlow[3 + j, ny : ny + 8])
        place(dx, nx + 2 + j, xhigh[3 + j, 0:ny], xhigh[3 + j, ny : ny + 8])
    at_row = iota((rows, 256), 0)
    side = jnp.where(at_row < 8, edge[2], jnp.where(at_row >= 8 + ny, edge[3], 1.0))
    keep[...] = jnp.where(iota((rows, 256), 1) < nz, side, 0.0)

    def applied(field, at, shift_at, base):
        mid = field[at]
        beside = field[at - 1] + field[at + 1]
        beside = beside + (pltpu.roll(mid, 1, 0) + pltpu.roll(mid, rows - 1, 0))
        beside = beside + (pltpu.roll(mid, 1, 1) + pltpu.roll(mid, 255, 1))
        return (dx[shift_at] + base) * mid - beside

    def folded(a):
        return jnp.sum(a[8 : 8 + ny].reshape(ny // 8, 8, 256), axis=0)

    def total(a):
        return jnp.sum(a, axis=(0, 1), keepdims=True)

    def probe(i, carry):
        mid = u0[4 * i + 3] * keep[...]
        return carry[0] + folded(mid * mid), carry[1] + folded(mid * applied(u0, 4 * i + 3, 4 * i + 2, 6.0))

    zero = jnp.zeros((8, 256), F32)
    norm, lift = lax.fori_loop(0, nx // 4, probe, (zero, zero))
    norm = total(norm)
    lift = total(lift)
    shift = jnp.where(norm > 0.0, lift / jnp.where(norm > 0.0, norm, 1.0), SHIFT)
    shift = to_grain(jnp.clip(shift, 0.0, 14.0))
    base = 6.0 - shift

    def along(i, count):
        return jnp.where(i < count, edge[0], jnp.where(i >= nx + count, edge[1], 1.0))

    def first(i, carry):
        u1[i] = applied(u0, i + 1, i, base) * (keep[...] * along(i, 2))
        return carry

    def second(i, carry):
        u2[i] = applied(u1, i + 1, i + 1, base) * (keep[...] * along(i, 1))
        return carry

    def third(i, carry):
        new = applied(u2, i + 1, i + 2, base) * keep[...]
        u3[i] = new[8 : 8 + ny]
        f0 = u0[i + 3]
        f1 = u1[i + 2]
        f2 = u2[i + 1]
        return (
            carry[0] + folded(f0 * f0),
            carry[1] + folded(f0 * f1),
            carry[2] + folded(f1 * f1),
            carry[3] + folded(f1 * f2),
            carry[4] + folded(f2 * f2),
            carry[5] + folded(f2 * new),
        )

    lax.fori_loop(0, nx + 4, first, 0)
    lax.fori_loop(0, nx + 2, second, 0)
    sums = lax.fori_loop(0, nx, third, (zero,) * 6)
    sums = [jnp.broadcast_to(total(a), (8, 128)) for a in sums]
    step = jnp.broadcast_to(shift, (8, 128)) - SHIFT
    pairs = translated([(a, jnp.zeros((8, 128), F32)) for a in sums], step)
    lane = iota((8, 128), 1)
    line = jnp.zeros((8, 128), F32)
    for k, (high, low) in enumerate(pairs):
        line = jnp.where(lane == k, high, jnp.where(lane == k + 6, low, line))
    for k in range(row_out.shape[0] // 8):
        row_out[8 * k : 8 * k + 8, :] = line
    c_out[...] = jnp.broadcast_to(shift, (8, 128))


def gathered(rows):
    parts = [(rows[8 * k : 8 * k + 8], jnp.zeros((8, 128), F32)) for k in range(rows.shape[0] // 8)]

    def joined(one, two):
        s, e = two_sum(one[0], two[0])
        return s, e + (one[1] + two[1])

    while len(parts) > 1:
        parts = [joined(*parts[k : k + 2]) if k + 1 < len(parts) else parts[k] for k in range(0, len(parts), 2)]
    s, e = parts[0]
    for by in (4, 2, 1):
        s, e = joined((s, e), (pltpu.roll(s, by, 0), pltpu.roll(e, by, 0)))
    lane = iota((8, 128), 1)
    return jnp.where(lane < 6, s, s + pltpu.roll(e, 6, 1))


def regroup(rows, out):
    line = gathered(rows)
    for k in range(out.shape[0] // 8):
        out[8 * k : 8 * k + 8, :] = line


def steps_of(moments, centre):
    def form(one, two):
        out = 0.0
        for k in range(len(one) + len(two) - 1):
            part = 0.0
            for i in range(len(one)):
                if 0 <= k - i < len(two):
                    part = part + one[i] * two[k - i]
            out = out + part * moments[k]
        return out

    def plus(one, factor, two):
        size = max(len(one), len(two))
        out = []
        for k in range(size):
            if k >= len(two):
                out.append(one[k])
            elif k >= len(one):
                out.append(factor * two[k])
            else:
                out.append(one[k] + factor * two[k])
        return out

    unit = jnp.ones_like(moments[0])
    residual = [unit]
    solution_field = []
    s = []
    p = []
    for step in range(3):
        raised = [residual[0] * centre]
        for k in range(1, len(residual)):
            raised.append(residual[k - 1] + centre * residual[k])
        raised.append(residual[-1])
        gamma = form(residual, residual)
        delta = form(residual, raised)
        if step == 0:
            alpha = gamma / delta
            s, p = raised, residual
        else:
            beta = gamma / gamma_prev
            alpha = gamma / (delta - beta * gamma / alpha_prev)
            s = plus(raised, beta, s)
            p = plus(residual, beta, p)
        solution_field = plus(solution_field, alpha, p)
        residual = plus(residual, -alpha, s)
        gamma_prev = gamma
        alpha_prev = alpha
    return solution_field, residual


def recentred(coefficients, step):
    out = list(coefficients)
    size = len(out)
    for i in range(size - 1):
        for k in range(size - 2, i - 1, -1):
            out[k] = out[k] + step * out[k + 1]
    return out


def finish(rows, c_in, b, u1, u2, u3, solution_field, residual, coef):
    nz = b.shape[2]
    i = pl.program_id(0)
    block = b.shape[0]

    @pl.when(i == 0)
    def _():
        line = gathered(rows)
        lane = lambda k: jnp.broadcast_to(jnp.sum(jnp.where(iota((8, 128), 1) == k, line, 0.0), axis=1, keepdims=True), (8, 128))
        moments = [(lane(k), lane(k + 6)) for k in range(6)]
        away = to_grain(moments[1][0] / moments[0][0])
        moments = [high + low for high, low in translated(moments, -away)]
        centre = SHIFT + away
        xs, rs = steps_of(moments, centre)
        step = c_in[...] - centre
        xs = recentred(xs, step)
        rs = recentred(rs, step)
        for k, value in enumerate(xs + rs):
            coef[k] = value

    def coefficient(k):
        return coef[k, 0:1, 0:1]

    for j in range(block):
        at = i * block + j
        f0 = b[j]
        f1 = u1[at + 2, 8:-8, 0:nz]
        f2 = u2[at + 1, 8:-8, 0:nz]
        f3 = u3[at, :, 0:nz]
        solution_field[j] = coefficient(0) * f0 + coefficient(1) * f1 + coefficient(2) * f2
        residual[j] = coefficient(3) * f0 + coefficient(4) * f1 + coefficient(5) * f2 + coefficient(6) * f3


def shifted(a, axis, by):
    count = lax.axis_size(axis)
    pairs = [(k, k + by) for k in range(count) if 0 <= k + by < count]
    return lax.ppermute(a, axis, pairs)


def spread(rows, axes):
    count = lax.axis_size(axes)
    out = lax.all_to_all(rows[:count].reshape(count, 1, 128), axes, 0, 0, tiled=True)
    return jnp.pad(out.reshape(count, 128), ((0, -count % 8), (0, 0)))


VMEM = pl.BlockSpec(memory_space=pltpu.VMEM)
SMEM = pl.BlockSpec(memory_space=pltpu.SMEM)


def call(body, out_shapes, count, scratch=(), smem=0, name=None):
    return pl.pallas_call(
        body,
        out_shape=out_shapes,
        in_specs=[SMEM] * smem + [VMEM] * (count - smem),
        out_specs=[VMEM] * len(out_shapes),
        scratch_shapes=list(scratch),
        compiler_params=pltpu.CompilerParams(vmem_limit_bytes=GRANT),
        name=name,
    )


def on_device(right_side, diagonal):
    nx, ny, nz = right_side.shape
    rows = ny + 16
    shape = lambda *dims: pltpu.VMEM(dims, F32)
    yf, yb = call(pack_y, (shape(nx, 8, nz),) * 2, 2, name="pack_y")(right_side, diagonal)
    ylow = shifted(yf, "z", 1)
    yhigh = shifted(yb, "z", -1)
    xf, xb = call(pack_x, (shape(5, ny + 8, nz),) * 2, 4, name="pack_x")(right_side, diagonal, ylow, yhigh)
    xlow = shifted(xf, GX, 1)
    xhigh = shifted(xb, GX, -1)
    gx = lax.axis_index(GX)
    gy = lax.axis_index("z")
    edge = jnp.stack(
        [gx > 0, gx < lax.axis_size(GX) - 1, gy > 0, gy < lax.axis_size("z") - 1]
    ).astype(F32)
    up = lambda n: -(-n // 8) * 8
    one = lax.axis_size(FIRST)
    two = lax.axis_size(SECOND)
    u1, u2, u3, line, shift = call(
        fields,
        (shape(nx + 4, rows, 256), shape(nx + 2, rows, 256), shape(nx, ny, 256), shape(up(one), 128), shape(8, 128)),
        7,
        scratch=(pltpu.VMEM((nx + 6, rows, 256), F32), pltpu.VMEM((nx + 4, rows, 256), F32), pltpu.VMEM((rows, 256), F32)),
        smem=1,
        name="fields",
    )(edge, right_side, diagonal, ylow, yhigh, xlow, xhigh)
    line = spread(line, FIRST)
    (line,) = call(regroup, (shape(up(two), 128),), 1, name="regroup")(line)
    line = spread(line, SECOND)
    block = 2
    tile = pl.BlockSpec((block, ny, nz), lambda i: (i, 0, 0))
    return pl.pallas_call(
        finish,
        out_shape=(jax.ShapeDtypeStruct((nx, ny, nz), F32),) * 2,
        grid=(nx // block,),
        in_specs=[VMEM, VMEM, tile, VMEM, VMEM, VMEM],
        out_specs=[tile, tile],
        scratch_shapes=[pltpu.VMEM((7, 8, 128), F32)],
        compiler_params=pltpu.CompilerParams(vmem_limit_bytes=GRANT),
        name="finish",
    )(line, shift, right_side, u1, u2, u3)


def solution_on(mesh, split):
    torus = Mesh(mesh.devices.reshape(*split, mesh.shape["gy"]), GX + ("z",))
    placed = (P(GX, "z", None), P(GX, "z", None))
    return jax.shard_map(on_device, mesh=torus, in_specs=placed, out_specs=placed, check_vma=False)


def solution(mesh):
    return solution_on(mesh, (8, 4, 2))
```

```python
import jax
import jax.numpy as jnp
from jax import lax
from jax.experimental import pallas as pl
from jax.experimental.pallas import tpu as pltpu
from jax.sharding import Mesh
from jax.sharding import PartitionSpec as P


SHIFT = 7.0
GRAIN = 8.0
GX = ("y", "x", "c")
FIRST = ("y", "c")
SECOND = ("x", "z")
F32 = jnp.float32
GRANT = 24 << 20
PARTS = 4


def two_sum(a, b):
    s = a + b
    t = s - a
    return s, (a - (s - t)) + (b - t)


def halves(a):
    t = a * 4097.0
    high = t - (t - a)
    return high, a - high


def scaled(pair, factor):
    high, low = halves(pair[0])
    s, e = two_sum(high * factor, low * factor)
    return s, e + pair[1] * factor


def added(one, two):
    s, e = two_sum(one[0], two[0])
    return two_sum(s, e + (one[1] + two[1]))


def translated(moments, step):
    row = list(moments)
    out = [row[0]]
    while len(row) > 1:
        row = [added(row[k + 1], scaled(row[k], step)) for k in range(len(row) - 1)]
        out.append(row[0])
    return out


def to_grain(x):
    return jnp.floor(x * GRAIN + 0.5) / GRAIN


def iota(shape, dim):
    return lax.broadcasted_iota(jnp.int32, shape, dim)


def place():
    gx = lax.axis_index(GX)
    gy = lax.axis_index("z")
    is_there = lambda x: x.astype(jnp.int32)
    return (
        lax.axis_index("c"),
        is_there(gx > 0),
        is_there(gx < lax.axis_size(GX) - 1),
        is_there(gy > 0),
        is_there(gy < lax.axis_size("z") - 1),
    )


def half_turn(a):
    return pltpu.roll(a, 64, a.ndim - 1)


def squeeze(first, second):
    left = lax.broadcasted_iota(jnp.int32, first.shape, first.ndim - 1) < 64
    return jnp.where(left, first, half_turn(second))


def lanes(block):
    rest = jnp.pad(block[..., 128:], ((0, 0),) * (block.ndim - 1) + ((0, 64),))
    return block[..., :128], rest


def pack(b, d, u0, dx, yf, yb, off, on, sems):
    where = place()
    nx, ny, _ = b.shape
    copies = [
        pltpu.make_async_copy(source, target.at[3 : 3 + nx, 8 : 8 + ny, :], sems.at[k])
        for k, (source, target) in enumerate(((b, u0), (d, dx)))
    ]
    for copy in copies:
        copy.start()
    for copy in copies:
        copy.wait()
    half = nx // 2

    def y_face(row, first_row):
        field = u0[3 : 3 + nx, row : row + 8, :]
        shift = pltpu.roll(dx[3 : 3 + nx, row : row + 8, :], 4, 1)
        sub = iota(field.shape, 1)
        face = jnp.where(sub < 3 if first_row else sub >= 5, field, shift)
        main, rest = lanes(face)
        return main, squeeze(rest[:half], rest[half:])

    for out, row, first_row in ((yf, ny, False), (yb, 8, True)):
        main, rest = y_face(row, first_row)
        out[0:nx] = main
        out[nx : nx + half] = rest
    mid = ny // 2
    for out, high in ((off, where[0]), (on, 1 - where[0])):
        for j in range(5):
            if j < 3:
                slab = u0[3 + j + high * (nx - 3), 8 : 8 + ny, :]
            else:
                slab = dx[j + high * (nx - 2), 8 : 8 + ny, :]
            main, rest = lanes(slab)
            out[j, 0:ny, :] = main
            out[j, ny : ny + mid, :] = squeeze(rest[:mid], rest[mid:])


def unsqueeze(main, rest, second):
    rest = half_turn(rest) if second else rest
    return jnp.concatenate([main, rest[..., :64]], axis=-1)


def corners(u0_in, dx_in, ylow, yhigh, u0, dx, off, on):
    where = place()
    nx = u0.shape[0] - 6
    ny = u0.shape[1] - 16
    half = nx // 2
    for halo, row in ((ylow, 0), (yhigh, 8 + ny)):
        for k in (0, 1):
            part = slice(k * half, (k + 1) * half)
            tile = unsqueeze(halo[part], halo[nx : nx + half], k == 1)
            at = slice(3 + k * half, 3 + (k + 1) * half)
            u0[at, row : row + 8, :] = tile
            dx[at, row : row + 8, :] = pltpu.roll(tile, 4, 1)
    for out, high in ((off, where[0]), (on, 1 - where[0])):
        one = 3 + high * (nx - 1)
        two = 4 + high * (nx - 3)
        for j, (field, at) in enumerate(((u0, one), (u0, two), (dx, one))):
            low = field[at, 0:8, :]
            out[j] = jnp.where(iota(low.shape, 0) >= 4, low, field[at, 8 + ny : 16 + ny, :])


def stencil(field, dx, at, base):
    mid = field[at]
    rows = mid.shape[0]
    padded = jnp.pad(mid, ((0, 0), (0, 256 - mid.shape[1])))
    beside = field[at - 1] + field[at + 1]
    beside = beside + (pltpu.roll(mid, 1, 0) + pltpu.roll(mid, rows - 1, 0))
    across = pltpu.roll(padded, 1, 1) + pltpu.roll(padded, 255, 1)
    return (dx[at] + base) * mid - (beside + across[:, : mid.shape[1]])


def fold(a):
    rows = a.shape[0] - 16
    return jnp.sum(a[8 : 8 + rows].reshape(rows // 8, 8, a.shape[1]), axis=0)


def total(a):
    return jnp.broadcast_to(jnp.sum(a, axis=(0, 1), keepdims=True), (8, 128))


def side_mask(where, shape):
    rows = iota(shape, 0)
    low = jnp.full(shape, where[3].astype(F32))
    high = jnp.full(shape, where[4].astype(F32))
    return jnp.where(rows < 8, low, jnp.where(rows >= shape[0] - 8, high, 1.0))


def products(f0, f1, f2, f3):
    return tuple(fold(p) for p in (f0 * f0, f0 * f1, f1 * f1, f1 * f2, f2 * f2)) + (
        jnp.sum((f2[8:-8] * f3).reshape(-1, 8, f3.shape[1]), axis=0),
    )


def accumulated(sums, more):
    return tuple(a + b for a, b in zip(sums, more))


def middle(u0, dx, u1, u2, u3, sums_out, shift_out, keep):
    where = place()
    nx = u0.shape[0] - 6
    shape = u0.shape[1:]
    zero = jnp.zeros((8, shape[1]), F32)
    keep[...] = side_mask(where, shape)

    def probe(i, carry):
        at = 5 + 3 * i
        mid = u0[at]
        return carry[0] + fold(mid * mid), carry[1] + fold(mid * stencil(u0, dx, at, 6.0))

    norm, lift = lax.fori_loop(0, 4, probe, (zero, zero), unroll=2)
    norm = total(norm)
    lift = total(lift)
    shift = jnp.where(norm > 0.0, lift / jnp.where(norm > 0.0, norm, 1.0), SHIFT)
    shift = to_grain(jnp.clip(shift, 0.0, 14.0))
    shift_out[...] = shift
    base = 6.0 - shift[0:1, 0:1]

    def first(i, carry):
        u1[i] = stencil(u0, dx, i, base) * keep[...]
        return carry

    def second(i, carry):
        u2[i] = stencil(u1, dx, i, base) * keep[...]
        return carry

    def third(i, sums):
        new = stencil(u2, dx, i, base)[8:-8]
        u3[i - 3] = new
        return accumulated(sums, products(u0[i], u1[i], u2[i], new))

    lax.fori_loop(4, nx + 2, first, 0, unroll=2)
    lax.fori_loop(5, nx + 1, second, 0, unroll=2)
    sums = lax.fori_loop(6, nx, third, (zero,) * 6)
    for k in range(6):
        sums_out[k] = sums[k]


def rim(u0_in, dx_in, u1_in, u2_in, u3_in, sums_in, shift_in, off, on, coff, con, u0, dx, u1, u2, u3, row_out):
    where = place()
    nx = u0.shape[0] - 6
    ny = u0.shape[1] - 16
    mid = ny // 2
    shape = u0.shape[1:]
    for main, corner, high in ((off, coff, where[0]), (on, con, 1 - where[0])):
        for j in range(5):
            slab = main[j, 0:ny, :]
            rest = main[j, ny : ny + mid, :]
            top = unsqueeze(slab[:mid], rest, False)
            bottom = unsqueeze(slab[mid:], rest, True)
            field, at = (u0, j + high * (nx + 3)) if j < 3 else (dx, j - 2 + high * (nx + 2))
            field[at, 8 : 8 + mid, :] = top
            field[at, 8 + mid : 8 + ny, :] = bottom
        one = 2 + high * (nx + 1)
        two = 1 + high * (nx + 3)
        for j, (field, at) in enumerate(((u0, one), (u0, two), (dx, one))):
            tile = corner[j]
            field[at, 0:8, :] = tile
            field[at, 8 + ny : 16 + ny, :] = tile
    keep = side_mask(where, shape)
    shift = shift_in[...]
    base = 6.0 - shift[0:1, 0:1]
    low = where[1].astype(F32)
    high = where[2].astype(F32)

    def first(i, carry):
        u1[1 + i] = stencil(u0, dx, 1 + i, base) * (keep * jnp.where(i < 2, low, 1.0))
        u1[nx + 2 + i] = stencil(u0, dx, nx + 2 + i, base) * (keep * jnp.where(i > 0, high, 1.0))
        return carry

    def second(i, carry):
        u2[2 + i] = stencil(u1, dx, 2 + i, base) * (keep * jnp.where(i < 1, low, 1.0))
        u2[nx + 1 + i] = stencil(u1, dx, nx + 1 + i, base) * (keep * jnp.where(i > 1, high, 1.0))
        return carry

    def third(i, sums):
        for at in (3 + i, nx + i):
            new = stencil(u2, dx, at, base)[8:-8]
            u3[at - 3] = new
            sums = accumulated(sums, products(u0[at], u1[at], u2[at], new))
        return sums

    lax.fori_loop(0, 3, first, 0)
    lax.fori_loop(0, 3, second, 0)
    sums = lax.fori_loop(0, 3, third, tuple(sums_in[k] for k in range(6)))
    pairs = translated([(total(a), jnp.zeros((8, 128), F32)) for a in sums], shift - SHIFT)
    lane = iota((8, 128), 1)
    line = jnp.zeros((8, 128), F32)
    for k, (high_part, low_part) in enumerate(pairs):
        line = jnp.where(lane == k, high_part, jnp.where(lane == k + 6, low_part, line))
    for k in range(row_out.shape[0] // 8):
        row_out[8 * k : 8 * k + 8, :] = line


def gathered(rows):
    parts = [(rows[8 * k : 8 * k + 8], jnp.zeros((8, 128), F32)) for k in range(rows.shape[0] // 8)]

    def joined(one, two):
        s, e = two_sum(one[0], two[0])
        return s, e + (one[1] + two[1])

    while len(parts) > 1:
        parts = [joined(*parts[k : k + 2]) if k + 1 < len(parts) else parts[k] for k in range(0, len(parts), 2)]
    s, e = parts[0]
    for by in (4, 2, 1):
        s, e = joined((s, e), (pltpu.roll(s, by, 0), pltpu.roll(e, by, 0)))
    lane = iota((8, 128), 1)
    return jnp.where(lane < 6, s, s + pltpu.roll(e, 6, 1))


def regroup(rows, out):
    line = gathered(rows)
    for k in range(out.shape[0] // 8):
        out[8 * k : 8 * k + 8, :] = line


def steps_of(moments, centre):
    def form(one, two):
        out = 0.0
        for k in range(len(one) + len(two) - 1):
            part = 0.0
            for i in range(len(one)):
                if 0 <= k - i < len(two):
                    part = part + one[i] * two[k - i]
            out = out + part * moments[k]
        return out

    def plus(one, factor, two):
        size = max(len(one), len(two))
        out = []
        for k in range(size):
            if k >= len(two):
                out.append(one[k])
            elif k >= len(one):
                out.append(factor * two[k])
            else:
                out.append(one[k] + factor * two[k])
        return out

    unit = jnp.ones_like(moments[0])
    residual = [unit]
    solution_field = []
    s = []
    p = []
    for step in range(3):
        raised = [residual[0] * centre]
        for k in range(1, len(residual)):
            raised.append(residual[k - 1] + centre * residual[k])
        raised.append(residual[-1])
        gamma = form(residual, residual)
        delta = form(residual, raised)
        if step == 0:
            alpha = gamma / delta
            s, p = raised, residual
        else:
            beta = gamma / gamma_prev
            alpha = gamma / (delta - beta * gamma / alpha_prev)
            s = plus(raised, beta, s)
            p = plus(residual, beta, p)
        solution_field = plus(solution_field, alpha, p)
        residual = plus(residual, -alpha, s)
        gamma_prev = gamma
        alpha_prev = alpha
    return solution_field, residual


def recentred(coefficients, step):
    out = list(coefficients)
    size = len(out)
    for i in range(size - 1):
        for k in range(size - 2, i - 1, -1):
            out[k] = out[k] + step * out[k + 1]
    return out


def finish(rows, shift_in, u0, u1, u2, u3, solution_field, residual, xs_out, rs_out, sems):
    nx, ny, nz = u3.shape
    line = gathered(rows)

    def lane(k):
        one = jnp.where(iota((8, 128), 1) == k, line, 0.0)
        return jnp.broadcast_to(jnp.sum(one, axis=1, keepdims=True), (8, 128))

    moments = [(lane(k), lane(k + 6)) for k in range(6)]
    away = to_grain(moments[1][0] / moments[0][0])
    moments = [high + low for high, low in translated(moments, -away)]
    centre = SHIFT + away
    xs, rs = steps_of(moments, centre)
    step = shift_in[...] - centre
    xs = [a[0:1, 0:1] for a in recentred(xs, step)]
    rs = [a[0:1, 0:1] for a in recentred(rs, step)]
    part = nx // PARTS
    copies = []
    for k in range(PARTS):

        def one(i, carry):
            f = (u0[i + 3, 8:-8, :], u1[i + 3, 8:-8, :], u2[i + 3, 8:-8, :], u3[i])
            xs_out[i] = xs[0] * f[0] + xs[1] * f[1] + xs[2] * f[2]
            rs_out[i] = rs[0] * f[0] + rs[1] * f[1] + rs[2] * f[2] + rs[3] * f[3]
            return carry

        lax.fori_loop(k * part, (k + 1) * part, one, 0)
        piece = pl.ds(k * part, part)
        for j, (source, target) in enumerate(((xs_out, solution_field), (rs_out, residual))):
            copy = pltpu.make_async_copy(source.at[piece], target.at[piece], sems.at[2 * k + j])
            copy.start()
            copies.append(copy)
    for copy in copies:
        copy.wait()


def shifted(a, axis, by):
    count = lax.axis_size(axis)
    pairs = [(k, k + by) for k in range(count) if 0 <= k + by < count]
    return lax.ppermute(a, axis, pairs)


def swapped(a, first):
    count = lax.axis_size(GX)
    pairs = []
    for k in range(first, count - 1, 2):
        pairs += [(k, k + 1), (k + 1, k)]
    return lax.ppermute(a, GX, pairs)


def spread(rows, axes):
    count = lax.axis_size(axes)
    out = lax.all_to_all(rows[:count].reshape(count, 1, 128), axes, 0, 0, tiled=True)
    return jnp.pad(out.reshape(count, 128), ((0, -count % 8), (0, 0)))


IN_VMEM = pl.BlockSpec(memory_space=pltpu.VMEM)
IN_HBM = pl.BlockSpec(memory_space=pltpu.HBM)


def call(body, name, outs, ins, scratch=(), aliases=None, out_specs=None, flops=0):
    return pl.pallas_call(
        body,
        out_shape=outs,
        in_specs=ins,
        out_specs=out_specs or (IN_VMEM,) * len(outs),
        scratch_shapes=list(scratch),
        input_output_aliases=aliases or {},
        compiler_params=pltpu.CompilerParams(vmem_limit_bytes=GRANT),
        cost_estimate=pl.CostEstimate(flops=flops, bytes_accessed=0, transcendentals=0) if flops else None,
        name=name,
    )


def on_device(right_side, diagonal):
    nx, ny, nz = right_side.shape
    rows = ny + 16
    shape = lambda *dims: pltpu.VMEM(dims, F32)
    field = shape(nx + 6, rows, nz)
    y_face = shape(nx + nx // 2, 8, 128)
    x_face = shape(5, ny + ny // 2, 128)
    corner = shape(3, 8, nz)
    u0, dx, yf, yb, off, on = call(
        pack,
        "pack",
        (field, field, y_face, y_face, x_face, x_face),
        (IN_HBM, IN_HBM),
        scratch=(pltpu.SemaphoreType.DMA((2,)),),
    )(*(pltpu.with_memory_space_constraint(a, pltpu.HBM) for a in (right_side, diagonal)))
    ylow = shifted(yf, "z", 1)
    yhigh = shifted(yb, "z", -1)
    off = swapped(off, 1)
    on = swapped(on, 0)
    u0, dx, coff, con = call(
        corners,
        "corners",
        (field, field, corner, corner),
        (IN_VMEM,) * 4,
        aliases={0: 0, 1: 1},
    )(u0, dx, ylow, yhigh)
    coff = swapped(coff, 1)
    con = swapped(con, 0)
    u1, u2, u3, sums, shift = call(
        middle,
        "middle",
        (field, field, shape(nx, ny, nz), shape(6, 8, nz), shape(8, 128)),
        (IN_VMEM,) * 2,
        scratch=(pltpu.VMEM((rows, nz), F32),),
        flops=20_000_000,
    )(u0, dx)
    up = lambda n: -(-n // 8) * 8
    one = lax.axis_size(FIRST)
    two = lax.axis_size(SECOND)
    u0, dx, u1, u2, u3, line = call(
        rim,
        "rim",
        (field, field, field, field, shape(nx, ny, nz), shape(up(one), 128)),
        (IN_VMEM,) * 11,
        aliases={0: 0, 1: 1, 2: 2, 3: 3, 4: 4},
    )(u0, dx, u1, u2, u3, sums, shift, off, on, coff, con)
    line = spread(line, FIRST)
    (line,) = call(regroup, "regroup", (shape(up(two), 128),), (IN_VMEM,))(line)
    line = spread(line, SECOND)
    whole = jax.ShapeDtypeStruct((nx, ny, nz), F32)
    return call(
        finish,
        "finish",
        (whole, whole),
        (IN_VMEM,) * 6,
        scratch=(pltpu.VMEM((nx, ny, nz), F32),) * 2 + (pltpu.SemaphoreType.DMA((2 * PARTS,)),),
        out_specs=(IN_HBM,) * 2,
    )(line, shift, u0, u1, u2, u3)


def solution_on(mesh, split):
    torus = Mesh(mesh.devices.reshape(*split, mesh.shape["gy"]), GX + ("z",))
    placed = (P(GX, "z", None), P(GX, "z", None))
    return jax.shard_map(on_device, mesh=torus, in_specs=placed, out_specs=placed, check_vma=False)


def solution(mesh):
    return solution_on(mesh, (8, 4, 2))
```

```python
import jax
import jax.numpy as jnp
from jax import lax
from jax.experimental import pallas as pl
from jax.experimental.pallas import tpu as pltpu
from jax.sharding import Mesh
from jax.sharding import PartitionSpec as P


SHIFT = 7.0
GRAIN = 8.0
GX = ("y", "x", "c")
FIRST = ("c", "z")
SECOND = ("y", "x")
F32 = jnp.float32
GRANT = 24 << 20
PARTS = 4


def two_sum(a, b):
    s = a + b
    t = s - a
    return s, (a - (s - t)) + (b - t)


def halves(a):
    t = a * 4097.0
    high = t - (t - a)
    return high, a - high


def scaled(pair, factor):
    high, low = halves(pair[0])
    s, e = two_sum(high * factor, low * factor)
    return s, e + pair[1] * factor


def added(one, two):
    s, e = two_sum(one[0], two[0])
    return two_sum(s, e + (one[1] + two[1]))


def translated(moments, step):
    row = list(moments)
    out = [row[0]]
    while len(row) > 1:
        row = [added(row[k + 1], scaled(row[k], step)) for k in range(len(row) - 1)]
        out.append(row[0])
    return out


def to_grain(x):
    return jnp.floor(x * GRAIN + 0.5) / GRAIN


def iota(shape, dim):
    return lax.broadcasted_iota(jnp.int32, shape, dim)


def place():
    gx = lax.axis_index(GX)
    gy = lax.axis_index("z")
    is_there = lambda x: x.astype(jnp.int32)
    return (
        lax.axis_index("c"),
        is_there(gx > 0),
        is_there(gx < lax.axis_size(GX) - 1),
        is_there(gy > 0),
        is_there(gy < lax.axis_size("z") - 1),
    )


def half_turn(a):
    return pltpu.roll(a, 64, a.ndim - 1)


def squeeze(first, second):
    left = lax.broadcasted_iota(jnp.int32, first.shape, first.ndim - 1) < 64
    return jnp.where(left, first, half_turn(second))


def lanes(block):
    rest = jnp.pad(block[..., 128:], ((0, 0),) * (block.ndim - 1) + ((0, 64),))
    return block[..., :128], rest


def merged(tiles, turns, first_row):
    sub = iota(tiles[0].shape, 1)
    width = 8 // len(turns) if len(turns) > 2 else 3
    out = tiles[0]
    for k in range(1, len(turns)):
        here = pltpu.roll(tiles[k], turns[k], 1)
        start = (k * width) if first_row else (8 - width + turns[k]) % 8
        out = jnp.where((sub >= start) & (sub < start + width), here, out)
    return out


FIELD_TURNS = ((0, 5), (0, 3))
SHIFT_TURNS = (0, 2, 4, 6)


def pack_y(b, d, yf, yb, faces, sems):
    nx, ny, _ = b.shape
    copies = [
        pltpu.make_async_copy(source.at[:, row : row + 8, :], faces.at[k], sems.at[k])
        for k, (source, row) in enumerate(((b, ny - 8), (d, ny - 8), (b, 0), (d, 0)))
    ]
    for copy in copies:
        copy.start()
    for copy in copies:
        copy.wait()
    for side, out in enumerate((yf, yb)):
        field = faces[2 * side]
        shift = faces[2 * side + 1]
        field = merged([field[k * nx // 2 : (k + 1) * nx // 2] for k in range(2)], FIELD_TURNS[side], side == 1)
        shift = merged([shift[k * nx // 4 : (k + 1) * nx // 4] for k in range(4)], SHIFT_TURNS, side == 1)
        main, rest = lanes(jnp.concatenate([field, shift], axis=0))
        count = main.shape[0]
        out[0:count] = main
        out[count : count + count // 2] = squeeze(rest[: count // 2], rest[count // 2 :])


def load(b, d, yf, u0, dx, off, on, sems):
    where = place()
    nx, ny, _ = b.shape
    copies = [
        pltpu.make_async_copy(source, target.at[3 : 3 + nx, 8 : 8 + ny, :], sems.at[k])
        for k, (source, target) in enumerate(((b, u0), (d, dx)))
    ]
    for copy in copies:
        copy.start()
    for copy in copies:
        copy.wait()
    mid = ny // 2
    own = ny // 8
    for out, high in ((off, where[0]), (on, 1 - where[0])):
        for j in range(5):
            if j < 3:
                slab = u0[3 + j + high * (nx - 3), 8 : 8 + ny, :]
            else:
                slab = dx[j + high * (nx - 2), 8 : 8 + ny, :]
            main, rest = lanes(slab)
            at = j * (own + own // 2)
            out[at : at + own] = main.reshape(own, 8, 128)
            out[at + own : at + own + own // 2] = squeeze(rest[:mid], rest[mid:]).reshape(own // 2, 8, 128)


def unsqueeze(main, rest, second):
    rest = half_turn(rest) if second else rest
    return jnp.concatenate([main, rest[..., :64]], axis=-1)


def corners(u0_in, dx_in, off_in, on_in, ylow, yhigh, u0, dx, off, on):
    where = place()
    nx = u0.shape[0] - 6
    ny = u0.shape[1] - 16
    count = nx // 2 + nx // 4
    for side, (halo, row) in enumerate(((ylow, 0), (yhigh, 8 + ny))):
        rest = halo[count : count + count // 2]
        tiles = jnp.concatenate(
            [unsqueeze(halo[: count // 2], rest, False), unsqueeze(halo[count // 2 : count], rest, True)], axis=0
        )
        field = tiles[: nx // 2]
        shift = tiles[nx // 2 :]
        for k, turn in enumerate(FIELD_TURNS[side]):
            at = slice(3 + k * nx // 2, 3 + (k + 1) * nx // 2)
            u0[at, row : row + 8, :] = pltpu.roll(field, 8 - turn, 1) if turn else field
        for k, turn in enumerate(SHIFT_TURNS):
            at = slice(3 + k * nx // 4, 3 + (k + 1) * nx // 4)
            dx[at, row : row + 8, :] = pltpu.roll(shift, 8 - turn, 1) if turn else shift
    start = 5 * (ny // 8 + ny // 16)
    for out, high in ((off, where[0]), (on, 1 - where[0])):
        one = 3 + high * (nx - 1)
        two = 4 + high * (nx - 3)
        rests = []
        for j, (field, at) in enumerate(((u0, one), (u0, two), (dx, one))):
            low = field[at, 0:8, :]
            tile = jnp.where(iota(low.shape, 0) >= 4, low, field[at, 8 + ny : 16 + ny, :])
            main, rest = lanes(tile)
            out[start + j] = main
            rests.append(rest)
        out[start + 3] = squeeze(rests[0], rests[1])
        out[start + 4] = rests[2]


def stencil(field, dx, at, base):
    mid = field[at]
    rows = mid.shape[0]
    padded = jnp.pad(mid, ((0, 0), (0, 256 - mid.shape[1])))
    beside = field[at - 1] + field[at + 1]
    beside = beside + (pltpu.roll(mid, 1, 0) + pltpu.roll(mid, rows - 1, 0))
    across = pltpu.roll(padded, 1, 1) + pltpu.roll(padded, 255, 1)
    return (dx[at] + base) * mid - (beside + across[:, : mid.shape[1]])


def fold(a):
    rows = a.shape[0] - 16
    return jnp.sum(a[8 : 8 + rows].reshape(rows // 8, 8, a.shape[1]), axis=0)


def total(a):
    return jnp.broadcast_to(jnp.sum(a, axis=(0, 1), keepdims=True), (8, 128))


def side_mask(where, shape):
    rows = iota(shape, 0)
    low = jnp.full(shape, where[3].astype(F32))
    high = jnp.full(shape, where[4].astype(F32))
    return jnp.where(rows < 8, low, jnp.where(rows >= shape[0] - 8, high, 1.0))


def products(f0, f1, f2, f3):
    return tuple(fold(p) for p in (f0 * f0, f0 * f1, f1 * f1, f1 * f2, f2 * f2)) + (
        jnp.sum((f2[8:-8] * f3).reshape(-1, 8, f3.shape[1]), axis=0),
    )


def accumulated(sums, more):
    return tuple(a + b for a, b in zip(sums, more))


def middle(u0, dx, u1, u2, u3, sums_out, shift_out, keep):
    where = place()
    nx = u0.shape[0] - 6
    shape = u0.shape[1:]
    zero = jnp.zeros((8, shape[1]), F32)
    keep[...] = side_mask(where, shape)

    def probe(i, carry):
        at = 5 + 3 * i
        mid = u0[at]
        return carry[0] + fold(mid * mid), carry[1] + fold(mid * stencil(u0, dx, at, 6.0))

    norm, lift = lax.fori_loop(0, 4, probe, (zero, zero), unroll=2)
    norm = total(norm)
    lift = total(lift)
    shift = jnp.where(norm > 0.0, lift / jnp.where(norm > 0.0, norm, 1.0), SHIFT)
    shift = to_grain(jnp.clip(shift, 0.0, 14.0))
    shift_out[...] = shift
    base = 6.0 - shift[0:1, 0:1]

    def first(i, carry):
        u1[i] = stencil(u0, dx, i, base) * keep[...]
        return carry

    def second(i, carry):
        u2[i] = stencil(u1, dx, i, base) * keep[...]
        return carry

    def third(i, sums):
        new = stencil(u2, dx, i, base)[8:-8]
        u3[i - 3] = new
        return accumulated(sums, products(u0[i], u1[i], u2[i], new))

    lax.fori_loop(4, nx + 2, first, 0, unroll=2)
    lax.fori_loop(5, nx + 1, second, 0, unroll=2)
    sums = lax.fori_loop(6, nx, third, (zero,) * 6)
    for k in range(6):
        sums_out[k] = sums[k]


def rim(u0_in, dx_in, u1_in, u2_in, u3_in, sums_in, shift_in, off, on, u0, dx, u1, u2, u3, row_out):
    where = place()
    nx = u0.shape[0] - 6
    ny = u0.shape[1] - 16
    mid = ny // 2
    shape = u0.shape[1:]
    own = ny // 8
    start = 5 * (own + own // 2)
    for face, high in ((off, where[0]), (on, 1 - where[0])):
        for j in range(5):
            begin = j * (own + own // 2)
            slab = face[begin : begin + own].reshape(ny, 128)
            rest = face[begin + own : begin + own + own // 2].reshape(mid, 128)
            top = unsqueeze(slab[:mid], rest, False)
            bottom = unsqueeze(slab[mid:], rest, True)
            field, at = (u0, j + high * (nx + 3)) if j < 3 else (dx, j - 2 + high * (nx + 2))
            field[at, 8 : 8 + mid, :] = top
            field[at, 8 + mid : 8 + ny, :] = bottom
        one = 2 + high * (nx + 1)
        two = 1 + high * (nx + 3)
        for j, (field, at) in enumerate(((u0, one), (u0, two), (dx, one))):
            tile = unsqueeze(face[start + j], face[start + 3 + j // 2], j == 1)
            field[at, 0:8, :] = tile
            field[at, 8 + ny : 16 + ny, :] = tile
    keep = side_mask(where, shape)
    shift = shift_in[...]
    base = 6.0 - shift[0:1, 0:1]
    low = where[1].astype(F32)
    high = where[2].astype(F32)

    def first(i, carry):
        u1[1 + i] = stencil(u0, dx, 1 + i, base) * (keep * jnp.where(i < 2, low, 1.0))
        u1[nx + 2 + i] = stencil(u0, dx, nx + 2 + i, base) * (keep * jnp.where(i > 0, high, 1.0))
        return carry

    def second(i, carry):
        u2[2 + i] = stencil(u1, dx, 2 + i, base) * (keep * jnp.where(i < 1, low, 1.0))
        u2[nx + 1 + i] = stencil(u1, dx, nx + 1 + i, base) * (keep * jnp.where(i > 1, high, 1.0))
        return carry

    def third(i, sums):
        for at in (3 + i, nx + i):
            new = stencil(u2, dx, at, base)[8:-8]
            u3[at - 3] = new
            sums = accumulated(sums, products(u0[at], u1[at], u2[at], new))
        return sums

    lax.fori_loop(0, 3, first, 0)
    lax.fori_loop(0, 3, second, 0)
    sums = lax.fori_loop(0, 3, third, tuple(sums_in[k] for k in range(6)))
    pairs = translated([(total(a), jnp.zeros((8, 128), F32)) for a in sums], shift - SHIFT)
    lane = iota((8, 128), 1)
    line = jnp.zeros((8, 128), F32)
    for k, (high_part, low_part) in enumerate(pairs):
        line = jnp.where(lane == k, high_part, jnp.where(lane == k + 6, low_part, line))
    for k in range(row_out.shape[0] // 8):
        row_out[8 * k : 8 * k + 8, :] = line


def gathered(rows):
    parts = [(rows[8 * k : 8 * k + 8], jnp.zeros((8, 128), F32)) for k in range(rows.shape[0] // 8)]

    def joined(one, two):
        s, e = two_sum(one[0], two[0])
        return s, e + (one[1] + two[1])

    while len(parts) > 1:
        parts = [joined(*parts[k : k + 2]) if k + 1 < len(parts) else parts[k] for k in range(0, len(parts), 2)]
    s, e = parts[0]
    for by in (4, 2, 1):
        s, e = joined((s, e), (pltpu.roll(s, by, 0), pltpu.roll(e, by, 0)))
    lane = iota((8, 128), 1)
    return jnp.where(lane < 6, s, s + pltpu.roll(e, 6, 1))


def regroup(rows, out):
    line = gathered(rows)
    for k in range(out.shape[0] // 8):
        out[8 * k : 8 * k + 8, :] = line


def steps_of(moments, centre):
    def form(one, two):
        out = 0.0
        for k in range(len(one) + len(two) - 1):
            part = 0.0
            for i in range(len(one)):
                if 0 <= k - i < len(two):
                    part = part + one[i] * two[k - i]
            out = out + part * moments[k]
        return out

    def plus(one, factor, two):
        size = max(len(one), len(two))
        out = []
        for k in range(size):
            if k >= len(two):
                out.append(one[k])
            elif k >= len(one):
                out.append(factor * two[k])
            else:
                out.append(one[k] + factor * two[k])
        return out

    unit = jnp.ones_like(moments[0])
    residual = [unit]
    solution_field = []
    s = []
    p = []
    for step in range(3):
        raised = [residual[0] * centre]
        for k in range(1, len(residual)):
            raised.append(residual[k - 1] + centre * residual[k])
        raised.append(residual[-1])
        gamma = form(residual, residual)
        delta = form(residual, raised)
        if step == 0:
            alpha = gamma / delta
            s, p = raised, residual
        else:
            beta = gamma / gamma_prev
            alpha = gamma / (delta - beta * gamma / alpha_prev)
            s = plus(raised, beta, s)
            p = plus(residual, beta, p)
        solution_field = plus(solution_field, alpha, p)
        residual = plus(residual, -alpha, s)
        gamma_prev = gamma
        alpha_prev = alpha
    return solution_field, residual


def recentred(coefficients, step):
    out = list(coefficients)
    size = len(out)
    for i in range(size - 1):
        for k in range(size - 2, i - 1, -1):
            out[k] = out[k] + step * out[k + 1]
    return out


def finish(rows, shift_in, u0, u1, u2, u3, solution_field, residual, xs_out, rs_out, sems):
    nx, ny, nz = u3.shape
    line = gathered(rows)

    def lane(k):
        one = jnp.where(iota((8, 128), 1) == k, line, 0.0)
        return jnp.broadcast_to(jnp.sum(one, axis=1, keepdims=True), (8, 128))

    moments = [(lane(k), lane(k + 6)) for k in range(6)]
    away = to_grain(moments[1][0] / moments[0][0])
    moments = [high + low for high, low in translated(moments, -away)]
    centre = SHIFT + away
    xs, rs = steps_of(moments, centre)
    step = shift_in[...] - centre
    xs = [a[0:1, 0:1] for a in recentred(xs, step)]
    rs = [a[0:1, 0:1] for a in recentred(rs, step)]
    part = nx // PARTS
    copies = []
    for k in range(PARTS):

        def one(i, carry):
            f = (u0[i + 3, 8:-8, :], u1[i + 3, 8:-8, :], u2[i + 3, 8:-8, :], u3[i])
            xs_out[i] = xs[0] * f[0] + xs[1] * f[1] + xs[2] * f[2]
            rs_out[i] = rs[0] * f[0] + rs[1] * f[1] + rs[2] * f[2] + rs[3] * f[3]
            return carry

        lax.fori_loop(k * part, (k + 1) * part, one, 0)
        piece = pl.ds(k * part, part)
        for j, (source, target) in enumerate(((xs_out, solution_field), (rs_out, residual))):
            copy = pltpu.make_async_copy(source.at[piece], target.at[piece], sems.at[2 * k + j])
            copy.start()
            copies.append(copy)
    for copy in copies:
        copy.wait()


def shifted(a, axis, by):
    count = lax.axis_size(axis)
    pairs = [(k, k + by) for k in range(count) if 0 <= k + by < count]
    return lax.ppermute(a, axis, pairs)


def swapped(a, first):
    count = lax.axis_size(GX)
    pairs = []
    for k in range(first, count - 1, 2):
        pairs += [(k, k + 1), (k + 1, k)]
    return lax.ppermute(a, GX, pairs)


def spread(rows, axes):
    count = lax.axis_size(axes)
    out = lax.all_to_all(rows[:count].reshape(count, 1, 128), axes, 0, 0, tiled=True)
    return jnp.pad(out.reshape(count, 128), ((0, -count % 8), (0, 0)))


IN_VMEM = pl.BlockSpec(memory_space=pltpu.VMEM)
IN_HBM = pl.BlockSpec(memory_space=pltpu.HBM)


def call(body, name, outs, ins, scratch=(), aliases=None, out_specs=None, flops=0):
    return pl.pallas_call(
        body,
        out_shape=outs,
        in_specs=ins,
        out_specs=out_specs or (IN_VMEM,) * len(outs),
        scratch_shapes=list(scratch),
        input_output_aliases=aliases or {},
        compiler_params=pltpu.CompilerParams(vmem_limit_bytes=GRANT),
        cost_estimate=pl.CostEstimate(flops=flops, bytes_accessed=0, transcendentals=0) if flops else None,
        name=name,
    )


def on_device(right_side, diagonal):
    nx, ny, nz = right_side.shape
    rows = ny + 16
    shape = lambda *dims: pltpu.VMEM(dims, F32)
    field = shape(nx + 6, rows, nz)
    y_face = shape((nx // 2 + nx // 4) * 3 // 2, 8, 128)
    x_face = shape(5 * (ny // 8 + ny // 16) + 5, 8, 128)
    right_side, diagonal = (pltpu.with_memory_space_constraint(a, pltpu.HBM) for a in (right_side, diagonal))
    yf, yb = call(
        pack_y,
        "pack_y",
        (y_face, y_face),
        (IN_HBM, IN_HBM),
        scratch=(pltpu.VMEM((4, nx, 8, nz), F32), pltpu.SemaphoreType.DMA((4,))),
    )(right_side, diagonal)
    ylow = shifted(yf, "z", 1)
    yhigh = shifted(yb, "z", -1)
    u0, dx, off, on = call(
        load,
        "load",
        (field, field, x_face, x_face),
        (IN_HBM, IN_HBM, IN_VMEM),
        scratch=(pltpu.SemaphoreType.DMA((2,)),),
        flops=10_000_000,
    )(right_side, diagonal, yf)
    u0, dx, off, on = call(
        corners,
        "corners",
        (field, field, x_face, x_face),
        (IN_VMEM,) * 6,
        aliases={k: k for k in range(4)},
    )(u0, dx, off, on, ylow, yhigh)
    off = swapped(off, 1)
    on = swapped(on, 0)
    u1, u2, u3, sums, shift = call(
        middle,
        "middle",
        (field, field, shape(nx, ny, nz), shape(6, 8, nz), shape(8, 128)),
        (IN_VMEM,) * 2,
        scratch=(pltpu.VMEM((rows, nz), F32),),
        flops=20_000_000,
    )(u0, dx)
    up = lambda n: -(-n // 8) * 8
    one = lax.axis_size(FIRST)
    two = lax.axis_size(SECOND)
    u0, dx, u1, u2, u3, line = call(
        rim,
        "rim",
        (field, field, field, field, shape(nx, ny, nz), shape(up(one), 128)),
        (IN_VMEM,) * 9,
        aliases={k: k for k in range(5)},
    )(u0, dx, u1, u2, u3, sums, shift, off, on)
    line = spread(line, FIRST)
    (line,) = call(regroup, "regroup", (shape(up(two), 128),), (IN_VMEM,))(line)
    line = spread(line, SECOND)
    whole = jax.ShapeDtypeStruct((nx, ny, nz), F32)
    return call(
        finish,
        "finish",
        (whole, whole),
        (IN_VMEM,) * 6,
        scratch=(pltpu.VMEM((nx, ny, nz), F32),) * 2 + (pltpu.SemaphoreType.DMA((2 * PARTS,)),),
        out_specs=(IN_HBM,) * 2,
    )(line, shift, u0, u1, u2, u3)


def solution_on(mesh, split):
    torus = Mesh(mesh.devices.reshape(*split, mesh.shape["gy"]), GX + ("z",))
    placed = (P(GX, "z", None), P(GX, "z", None))
    return jax.shard_map(on_device, mesh=torus, in_specs=placed, out_specs=placed, check_vma=False)


def solution(mesh):
    return solution_on(mesh, (8, 4, 2))
```

```python
import jax
import jax.numpy as jnp
from jax import lax
from jax.experimental import pallas as pl
from jax.experimental.pallas import tpu as pltpu
from jax.sharding import Mesh
from jax.sharding import PartitionSpec as P


SHIFT = 7.0
GRAIN = 8.0
GX = ("y", "x", "c")
FIRST = ("c", "z")
SECOND = ("y", "x")
F32 = jnp.float32
GRANT = 24 << 20
PARTS = 4
PART = 16
TOP = 16


def two_sum(a, b):
    s = a + b
    t = s - a
    return s, (a - (s - t)) + (b - t)


def halves(a):
    t = a * 4097.0
    high = t - (t - a)
    return high, a - high


def scaled(pair, factor):
    high, low = halves(pair[0])
    s, e = two_sum(high * factor, low * factor)
    return s, e + pair[1] * factor


def added(one, two):
    s, e = two_sum(one[0], two[0])
    return two_sum(s, e + (one[1] + two[1]))


def translated(moments, step):
    row = list(moments)
    out = [row[0]]
    while len(row) > 1:
        row = [added(row[k + 1], scaled(row[k], step)) for k in range(len(row) - 1)]
        out.append(row[0])
    return out


def to_grain(x):
    return jnp.floor(x * GRAIN + 0.5) / GRAIN


def iota(shape, dim):
    return lax.broadcasted_iota(jnp.int32, shape, dim)


def place():
    gx = lax.axis_index(GX)
    gy = lax.axis_index("z")
    is_there = lambda x: x.astype(jnp.int32)
    return (
        lax.axis_index("c"),
        is_there(gx > 0),
        is_there(gx < lax.axis_size(GX) - 1),
        is_there(gy > 0),
        is_there(gy < lax.axis_size("z") - 1),
    )


def half_turn(a):
    return pltpu.roll(a, 64, a.ndim - 1)


def squeeze(first, second):
    left = lax.broadcasted_iota(jnp.int32, first.shape, first.ndim - 1) < 64
    return jnp.where(left, first, half_turn(second))


def lanes(block):
    rest = jnp.pad(block[..., 128:], ((0, 0),) * (block.ndim - 1) + ((0, 64),))
    return block[..., :128], rest


def merged(tiles, turns, first_row):
    sub = iota(tiles[0].shape, 1)
    width = 8 // len(turns) if len(turns) > 2 else 3
    out = tiles[0]
    for k in range(1, len(turns)):
        here = pltpu.roll(tiles[k], turns[k], 1)
        start = (k * width) if first_row else (8 - width + turns[k]) % 8
        out = jnp.where((sub >= start) & (sub < start + width), here, out)
    return out


FIELD_TURNS = ((0, 5), (0, 3))
SHIFT_TURNS = (0, 2, 4, 6)


def pack_y(b, d, one, two, faces, sems):
    even = lax.axis_index("z") % 2 == 0
    nx, ny, _ = b.shape
    copies = [
        pltpu.make_async_copy(source.at[:, row : row + 8, :], faces.at[k], sems.at[k])
        for k, (source, row) in enumerate(((b, ny - 8), (d, ny - 8), (b, 0), (d, 0)))
    ]
    for copy in copies:
        copy.start()
    for copy in copies:
        copy.wait()
    done = []
    for side in range(2):
        field = faces[2 * side]
        shift = faces[2 * side + 1]
        field = merged([field[k * nx // 2 : (k + 1) * nx // 2] for k in range(2)], FIELD_TURNS[side], side == 1)
        shift = merged([shift[k * nx // 4 : (k + 1) * nx // 4] for k in range(4)], SHIFT_TURNS, side == 1)
        main, rest = lanes(jnp.concatenate([field, shift], axis=0))
        count = main.shape[0]
        done.append(jnp.concatenate([main, squeeze(rest[: count // 2], rest[count // 2 :])], axis=0))
    one[...] = jnp.where(even, done[0], done[1])
    two[...] = jnp.where(even, done[1], done[0])


def load(b, d, face, u0, dx, off, on, stage, sems):
    where = place()
    nx, ny, _ = b.shape
    copies = [pltpu.make_async_copy(source, stage.at[k], sems.at[k]) for k, source in enumerate((b, d))]
    for copy in copies:
        copy.start()
    for k, (copy, into) in enumerate(zip(copies, (u0, dx))):
        copy.wait()

        def one(i, carry):
            main, rest = lanes(stage[k, i])
            into[0, i + 3, TOP : TOP + ny, :] = main
            into[1, i + 3, TOP : TOP + ny, :] = rest
            return carry

        lax.fori_loop(0, nx, one, 0, unroll=2)
    mid = ny // 2
    own = ny // 8
    for out, high in ((off, where[0]), (on, 1 - where[0])):
        for j in range(5):
            into, slab = (u0, 3 + j + high * (nx - 3)) if j < 3 else (dx, j + high * (nx - 2))
            at = j * (own + own // 2)
            out[at : at + own] = into[0, slab, TOP : TOP + ny, :].reshape(own, 8, 128)
            rest = into[1, slab, TOP : TOP + ny, :]
            out[at + own : at + own + own // 2] = (rest[:mid] + half_turn(rest[mid:])).reshape(own // 2, 8, 128)


def lone(rest, second):
    rest = half_turn(rest) if second else rest
    return jnp.where(lax.broadcasted_iota(jnp.int32, rest.shape, rest.ndim - 1) < 64, rest, 0.0)


def corners(u0_in, dx_in, off_in, on_in, got_one, got_two, u0, dx, off, on):
    where = place()
    even = lax.axis_index("z") % 2 == 0
    nx = u0.shape[1] - 6
    ny = u0.shape[2] - 2 * TOP
    count = nx // 2 + nx // 4
    half = count // 2
    for side, row in enumerate((TOP - 8, TOP + ny)):
        first, second = (got_two, got_one) if side == 0 else (got_one, got_two)
        halo = jnp.where(even, first[...], second[...])
        rest = halo[count : count + half]
        for plane, tiles in enumerate((halo[:count], jnp.concatenate([lone(rest, False), lone(rest, True)], axis=0))):
            field = tiles[: nx // 2]
            shift = tiles[nx // 2 :]
            for k, turn in enumerate(FIELD_TURNS[side]):
                at = slice(3 + k * nx // 2, 3 + (k + 1) * nx // 2)
                u0[plane, at, row : row + 8, :] = pltpu.roll(field, 8 - turn, 1) if turn else field
            for k, turn in enumerate(SHIFT_TURNS):
                at = slice(3 + k * nx // 4, 3 + (k + 1) * nx // 4)
                dx[plane, at, row : row + 8, :] = pltpu.roll(shift, 8 - turn, 1) if turn else shift
    start = 5 * (ny // 8 + ny // 16)
    for out, high in ((off, where[0]), (on, 1 - where[0])):
        one = 3 + high * (nx - 1)
        two = 4 + high * (nx - 3)
        rests = []
        for j, (field, at) in enumerate(((u0, one), (u0, two), (dx, one))):
            tiles = []
            for plane in range(2):
                low = field[plane, at, TOP - 8 : TOP, :]
                tiles.append(jnp.where(iota(low.shape, 0) >= 4, low, field[plane, at, TOP + ny : TOP + ny + 8, :]))
            out[start + j] = tiles[0]
            rests.append(tiles[1])
        out[start + 3] = squeeze(rests[0], rests[1])
        out[start + 4] = rests[2]


def stencil(field, dx, at, base, row, rows):
    here = slice(row, row + rows)
    above = slice(row - 1, row + rows - 1)
    below = slice(row + 1, row + rows + 1)
    lane = iota((rows, 128), 1)
    mid = [field[p, at, here, :] for p in range(2)]
    beside = [
        (field[p, at - 1, here, :] + field[p, at + 1, here, :]) + (field[p, at, above, :] + field[p, at, below, :])
        for p in range(2)
    ]
    right = [pltpu.roll(a, 1, 1) for a in mid]
    left = [pltpu.roll(a, 127, 1) for a in mid]
    across = (
        jnp.where(lane == 0, right[1], right[0]) + jnp.where(lane == 127, left[1], left[0]),
        jnp.where(lane == 0, right[0], right[1]) + left[1],
    )
    new = [(dx[p, at, here, :] + base) * mid[p] - (beside[p] + across[p]) for p in range(2)]
    return new[0], jnp.where(lane < 64, new[1], 0.0)


def fold(a):
    return jnp.sum(a.reshape(-1, 8, 128), axis=0)


def total(a):
    return jnp.broadcast_to(jnp.sum(a, axis=(0, 1), keepdims=True), (8, 128))


def raised(into, field, dx, at, base, there, factor=None):
    ny = field.shape[2] - 2 * TOP
    for row in range(TOP, TOP + ny, PART):
        for p, new in enumerate(stencil(field, dx, at, base, row, PART)):
            into[p, at, row : row + PART, :] = new if factor is None else new * factor
    for row, edge in ((TOP - 8, there[0]), (TOP + ny, there[1])):
        edge = edge if factor is None else edge * factor
        for p, new in enumerate(stencil(field, dx, at, base, row, 8)):
            into[p, at, row : row + 8, :] = new * edge


def summed(u0, dx, u1, u2, u3, at, base, sums):
    ny = u0.shape[2] - 2 * TOP
    sums = list(sums)
    for row in range(TOP, TOP + ny, PART):
        here = slice(row, row + PART)
        for p, f3 in enumerate(stencil(u2, dx, at, base, row, PART)):
            u3[p, at - 3, row - TOP : row - TOP + PART, :] = f3
            f0 = u0[p, at, here, :]
            f1 = u1[p, at, here, :]
            f2 = u2[p, at, here, :]
            for k, product in enumerate((f0 * f0, f0 * f1, f1 * f1, f1 * f2, f2 * f2, f2 * f3)):
                sums[k] = sums[k] + fold(product)
    return tuple(sums)


def middle(u0, dx, u1, u2, u3, sums_out, shift_out):
    where = place()
    nx = u0.shape[1] - 6
    ny = u0.shape[2] - 2 * TOP
    there = [where[k].astype(F32) for k in (3, 4)]
    zero = jnp.zeros((8, 128), F32)

    def probe(i, carry):
        norm, lift = carry
        at = 5 + 3 * i
        for row in range(TOP, TOP + ny, PART):
            for p, new in enumerate(stencil(u0, dx, at, 6.0, row, PART)):
                mid = u0[p, at, row : row + PART, :]
                norm = norm + fold(mid * mid)
                lift = lift + fold(mid * new)
        return norm, lift

    norm, lift = lax.fori_loop(0, 4, probe, (zero, zero), unroll=2)
    norm = total(norm)
    lift = total(lift)
    shift = jnp.where(norm > 0.0, lift / jnp.where(norm > 0.0, norm, 1.0), SHIFT)
    shift = to_grain(jnp.clip(shift, 0.0, 14.0))
    shift_out[...] = shift
    base = 6.0 - shift[0:1, :]

    def first(i, carry):
        raised(u1, u0, dx, i, base, there)
        return carry

    def second(i, carry):
        raised(u2, u1, dx, i, base, there)
        return carry

    def third(i, sums):
        return summed(u0, dx, u1, u2, u3, i, base, sums)

    lax.fori_loop(4, nx + 2, first, 0, unroll=2)
    lax.fori_loop(5, nx + 1, second, 0, unroll=2)
    sums = lax.fori_loop(6, nx, third, (zero,) * 6)
    for k in range(6):
        sums_out[k] = sums[k]


def rim(u0_in, dx_in, u1_in, u2_in, u3_in, sums_in, shift_in, off, on, u0, dx, u1, u2, u3, row_out):
    where = place()
    nx = u0.shape[1] - 6
    ny = u0.shape[2] - 2 * TOP
    there = [where[k].astype(F32) for k in (3, 4)]
    mid = ny // 2
    own = ny // 8
    start = 5 * (own + own // 2)
    for face, high in ((off, where[0]), (on, 1 - where[0])):
        for j in range(5):
            begin = j * (own + own // 2)
            rest = face[begin + own : begin + own + own // 2].reshape(mid, 128)
            field, at = (u0, j + high * (nx + 3)) if j < 3 else (dx, j - 2 + high * (nx + 2))
            field[0, at, TOP : TOP + ny, :] = face[begin : begin + own].reshape(ny, 128)
            field[1, at, TOP : TOP + mid, :] = lone(rest, False)
            field[1, at, TOP + mid : TOP + ny, :] = lone(rest, True)
        one = 2 + high * (nx + 1)
        two = 1 + high * (nx + 3)
        for j, (field, at) in enumerate(((u0, one), (u0, two), (dx, one))):
            for plane, tile in enumerate((face[start + j], lone(face[start + 3 + j // 2], j == 1))):
                field[plane, at, TOP - 8 : TOP, :] = tile
                field[plane, at, TOP + ny : TOP + ny + 8, :] = tile
    shift = shift_in[...]
    base = 6.0 - shift[0:1, :]
    low = where[1].astype(F32)
    high = where[2].astype(F32)

    def first(i, carry):
        raised(u1, u0, dx, 1 + i, base, there, jnp.where(i < 2, low, 1.0))
        raised(u1, u0, dx, nx + 2 + i, base, there, jnp.where(i > 0, high, 1.0))
        return carry

    def second(i, carry):
        raised(u2, u1, dx, 2 + i, base, there, jnp.where(i < 1, low, 1.0))
        raised(u2, u1, dx, nx + 1 + i, base, there, jnp.where(i > 1, high, 1.0))
        return carry

    def third(i, sums):
        for at in (3 + i, nx + i):
            sums = summed(u0, dx, u1, u2, u3, at, base, sums)
        return sums

    lax.fori_loop(0, 3, first, 0)
    lax.fori_loop(0, 3, second, 0)
    sums = lax.fori_loop(0, 3, third, tuple(sums_in[k] for k in range(6)))
    pairs = translated([(total(a), jnp.zeros((8, 128), F32)) for a in sums], shift - SHIFT)
    lane = iota((8, 128), 1)
    line = jnp.zeros((8, 128), F32)
    for k, (high_part, low_part) in enumerate(pairs):
        line = jnp.where(lane == k, high_part, jnp.where(lane == k + 6, low_part, line))
    for k in range(row_out.shape[0] // 8):
        row_out[8 * k : 8 * k + 8, :] = line


def gathered(rows):
    parts = [(rows[8 * k : 8 * k + 8], jnp.zeros((8, 128), F32)) for k in range(rows.shape[0] // 8)]

    def joined(one, two):
        s, e = two_sum(one[0], two[0])
        return s, e + (one[1] + two[1])

    while len(parts) > 1:
        parts = [joined(*parts[k : k + 2]) if k + 1 < len(parts) else parts[k] for k in range(0, len(parts), 2)]
    s, e = parts[0]
    for by in (4, 2, 1):
        s, e = joined((s, e), (pltpu.roll(s, by, 0), pltpu.roll(e, by, 0)))
    lane = iota((8, 128), 1)
    return jnp.where(lane < 6, s, s + pltpu.roll(e, 6, 1))


def regroup(rows, out):
    line = gathered(rows)
    for k in range(out.shape[0] // 8):
        out[8 * k : 8 * k + 8, :] = line


def steps_of(moments, centre):
    def form(one, two):
        out = 0.0
        for k in range(len(one) + len(two) - 1):
            part = 0.0
            for i in range(len(one)):
                if 0 <= k - i < len(two):
                    part = part + one[i] * two[k - i]
            out = out + part * moments[k]
        return out

    def plus(one, factor, two):
        size = max(len(one), len(two))
        out = []
        for k in range(size):
            if k >= len(two):
                out.append(one[k])
            elif k >= len(one):
                out.append(factor * two[k])
            else:
                out.append(one[k] + factor * two[k])
        return out

    unit = jnp.ones_like(moments[0])
    residual = [unit]
    solution_field = []
    s = []
    p = []
    for step in range(3):
        raised = [residual[0] * centre]
        for k in range(1, len(residual)):
            raised.append(residual[k - 1] + centre * residual[k])
        raised.append(residual[-1])
        gamma = form(residual, residual)
        delta = form(residual, raised)
        if step == 0:
            alpha = gamma / delta
            s, p = raised, residual
        else:
            beta = gamma / gamma_prev
            alpha = gamma / (delta - beta * gamma / alpha_prev)
            s = plus(raised, beta, s)
            p = plus(residual, beta, p)
        solution_field = plus(solution_field, alpha, p)
        residual = plus(residual, -alpha, s)
        gamma_prev = gamma
        alpha_prev = alpha
    return solution_field, residual


def recentred(coefficients, step):
    out = list(coefficients)
    size = len(out)
    for i in range(size - 1):
        for k in range(size - 2, i - 1, -1):
            out[k] = out[k] + step * out[k + 1]
    return out


def finish(rows, shift_in, u0, u1, u2, u3, solution_field, residual, xs_out, rs_out, sems):
    nx, ny, nz = xs_out.shape
    line = gathered(rows)

    def lane(k):
        one = jnp.where(iota((8, 128), 1) == k, line, 0.0)
        return jnp.broadcast_to(jnp.sum(one, axis=1, keepdims=True), (8, 128))

    moments = [(lane(k), lane(k + 6)) for k in range(6)]
    away = to_grain(moments[1][0] / moments[0][0])
    moments = [high + low for high, low in translated(moments, -away)]
    centre = SHIFT + away
    xs, rs = steps_of(moments, centre)
    step = shift_in[...] - centre
    xs = [a[0:1, :] for a in recentred(xs, step)]
    rs = [a[0:1, :] for a in recentred(rs, step)]
    part = nx // PARTS
    copies = []
    for k in range(PARTS):

        def one(i, carry):
            for p, (begin, width) in enumerate(((0, 128), (128, nz - 128))):
                own = pl.ds(TOP, ny)
                f = (u0[p, i + 3, own, :], u1[p, i + 3, own, :], u2[p, i + 3, own, :], u3[p, i])
                x = (xs[0] * f[0] + xs[1] * f[1]) + xs[2] * f[2]
                r = (rs[0] * f[0] + rs[1] * f[1]) + (rs[2] * f[2] + rs[3] * f[3])
                xs_out[i, :, begin : begin + width] = x[:, :width]
                rs_out[i, :, begin : begin + width] = r[:, :width]
            return carry

        lax.fori_loop(k * part, (k + 1) * part, one, 0)
        piece = pl.ds(k * part, part)
        for j, (source, target) in enumerate(((xs_out, solution_field), (rs_out, residual))):
            copy = pltpu.make_async_copy(source.at[piece], target.at[piece], sems.at[2 * k + j])
            copy.start()
            copies.append(copy)
    for copy in copies:
        copy.wait()


def swapped(a, axis, first):
    count = lax.axis_size(axis)
    pairs = []
    for k in range(first, count - 1, 2):
        pairs += [(k, k + 1), (k + 1, k)]
    return lax.ppermute(a, axis, pairs)


def spread(rows, axes):
    count = lax.axis_size(axes)
    out = lax.all_to_all(rows[:count].reshape(count, 1, 128), axes, 0, 0, tiled=True)
    return jnp.pad(out.reshape(count, 128), ((0, -count % 8), (0, 0)))


IN_VMEM = pl.BlockSpec(memory_space=pltpu.VMEM)
IN_HBM = pl.BlockSpec(memory_space=pltpu.HBM)


def call(body, name, outs, ins, scratch=(), aliases=None, out_specs=None, flops=0):
    return pl.pallas_call(
        body,
        out_shape=outs,
        in_specs=ins,
        out_specs=out_specs or (IN_VMEM,) * len(outs),
        scratch_shapes=list(scratch),
        input_output_aliases=aliases or {},
        compiler_params=pltpu.CompilerParams(vmem_limit_bytes=GRANT),
        cost_estimate=pl.CostEstimate(flops=flops, bytes_accessed=0, transcendentals=0) if flops else None,
        name=name,
    )


def on_device(right_side, diagonal):
    nx, ny, nz = right_side.shape
    rows = ny + 2 * TOP
    shape = lambda *dims: pltpu.VMEM(dims, F32)
    field = shape(2, nx + 6, rows, 128)
    y_face = shape((nx // 2 + nx // 4) * 3 // 2, 8, 128)
    x_face = shape(5 * (ny // 8 + ny // 16) + 5, 8, 128)
    right_side, diagonal = (pltpu.with_memory_space_constraint(a, pltpu.HBM) for a in (right_side, diagonal))
    y_one, y_two = call(
        pack_y,
        "pack_y",
        (y_face, y_face),
        (IN_HBM, IN_HBM),
        scratch=(pltpu.VMEM((4, nx, 8, nz), F32), pltpu.SemaphoreType.DMA((4,))),
    )(right_side, diagonal)
    got_one = swapped(y_one, "z", 0)
    got_two = swapped(y_two, "z", 1)
    u0, dx, off, on = call(
        load,
        "load",
        (field, field, x_face, x_face),
        (IN_HBM, IN_HBM, IN_VMEM),
        scratch=(pltpu.VMEM((2, nx, ny, nz), F32), pltpu.SemaphoreType.DMA((2,))),
        flops=10_000_000,
    )(right_side, diagonal, y_one)
    u0, dx, off, on = call(
        corners,
        "corners",
        (field, field, x_face, x_face),
        (IN_VMEM,) * 6,
        aliases={k: k for k in range(4)},
    )(u0, dx, off, on, got_one, got_two)
    off = swapped(off, GX, 1)
    on = swapped(on, GX, 0)
    u1, u2, u3, sums, shift = call(
        middle,
        "middle",
        (field, field, shape(2, nx, ny, 128), shape(6, 8, 128), shape(8, 128)),
        (IN_VMEM,) * 2,
        flops=20_000_000,
    )(u0, dx)
    up = lambda n: -(-n // 8) * 8
    one = lax.axis_size(FIRST)
    two = lax.axis_size(SECOND)
    u0, dx, u1, u2, u3, line = call(
        rim,
        "rim",
        (field, field, field, field, shape(2, nx, ny, 128), shape(up(one), 128)),
        (IN_VMEM,) * 9,
        aliases={k: k for k in range(5)},
    )(u0, dx, u1, u2, u3, sums, shift, off, on)
    line = spread(line, FIRST)
    (line,) = call(regroup, "regroup", (shape(up(two), 128),), (IN_VMEM,))(line)
    line = spread(line, SECOND)
    whole = jax.ShapeDtypeStruct((nx, ny, nz), F32)
    return call(
        finish,
        "finish",
        (whole, whole),
        (IN_VMEM,) * 6,
        scratch=(pltpu.VMEM((nx, ny, nz), F32),) * 2 + (pltpu.SemaphoreType.DMA((2 * PARTS,)),),
        out_specs=(IN_HBM,) * 2,
    )(line, shift, u0, u1, u2, u3)


def solution_on(mesh, split):
    torus = Mesh(mesh.devices.reshape(*split, mesh.shape["gy"]), GX + ("z",))
    placed = (P(GX, "z", None), P(GX, "z", None))
    return jax.shard_map(on_device, mesh=torus, in_specs=placed, out_specs=placed, check_vma=False)


def solution(mesh):
    return solution_on(mesh, (8, 4, 2))
```

```python
import jax
import jax.numpy as jnp
from jax import lax
from jax.experimental import pallas as pl
from jax.experimental.pallas import tpu as pltpu
from jax.sharding import Mesh
from jax.sharding import PartitionSpec as P


SHIFT = 7.0
GRAIN = 8.0
GX = ("y", "x", "c")
FIRST = ("c", "z")
SECOND = ("y", "x")
F32 = jnp.float32
GRANT = 24 << 20
PARTS = 4
PART = 16
TOP = 16


def two_sum(a, b):
    s = a + b
    t = s - a
    return s, (a - (s - t)) + (b - t)


def halves(a):
    t = a * 4097.0
    high = t - (t - a)
    return high, a - high


def scaled(pair, factor):
    high, low = halves(pair[0])
    s, e = two_sum(high * factor, low * factor)
    return s, e + pair[1] * factor


def added(one, two):
    s, e = two_sum(one[0], two[0])
    return two_sum(s, e + (one[1] + two[1]))


def translated(moments, step):
    row = list(moments)
    out = [row[0]]
    while len(row) > 1:
        row = [added(row[k + 1], scaled(row[k], step)) for k in range(len(row) - 1)]
        out.append(row[0])
    return out


def to_grain(x):
    return jnp.floor(x * GRAIN + 0.5) / GRAIN


def iota(shape, dim):
    return lax.broadcasted_iota(jnp.int32, shape, dim)


def place():
    gx = lax.axis_index(GX)
    gy = lax.axis_index("z")
    is_there = lambda x: x.astype(jnp.int32)
    return (
        lax.axis_index("c"),
        is_there(gx > 0),
        is_there(gx < lax.axis_size(GX) - 1),
        is_there(gy > 0),
        is_there(gy < lax.axis_size("z") - 1),
    )


def half_turn(a):
    return pltpu.roll(a, 64, a.ndim - 1)


def squeeze(first, second):
    left = lax.broadcasted_iota(jnp.int32, first.shape, first.ndim - 1) < 64
    return jnp.where(left, first, half_turn(second))


def lanes(block):
    rest = jnp.pad(block[..., 128:], ((0, 0),) * (block.ndim - 1) + ((0, 64),))
    return block[..., :128], rest


def merged(tiles, turns, first_row):
    sub = iota(tiles[0].shape, 1)
    width = 8 // len(turns) if len(turns) > 2 else 3
    out = tiles[0]
    for k in range(1, len(turns)):
        here = pltpu.roll(tiles[k], turns[k], 1)
        start = (k * width) if first_row else (8 - width + turns[k]) % 8
        out = jnp.where((sub >= start) & (sub < start + width), here, out)
    return out


FIELD_TURNS = ((0, 5), (0, 3))
SHIFT_TURNS = (0, 2, 4, 6)


def pack_y(b, d, one, two, faces, sems):
    even = lax.axis_index("z") % 2 == 0
    nx, ny, _ = b.shape
    copies = [
        pltpu.make_async_copy(source.at[:, row : row + 8, :], faces.at[k], sems.at[k])
        for k, (source, row) in enumerate(((b, ny - 8), (d, ny - 8), (b, 0), (d, 0)))
    ]
    for copy in copies:
        copy.start()
    for copy in copies:
        copy.wait()
    done = []
    for side in range(2):
        field = faces[2 * side]
        shift = faces[2 * side + 1]
        field = merged([field[k * nx // 2 : (k + 1) * nx // 2] for k in range(2)], FIELD_TURNS[side], side == 1)
        shift = merged([shift[k * nx // 4 : (k + 1) * nx // 4] for k in range(4)], SHIFT_TURNS, side == 1)
        main, rest = lanes(jnp.concatenate([field, shift], axis=0))
        count = main.shape[0]
        done.append(jnp.concatenate([main, squeeze(rest[: count // 2], rest[count // 2 :])], axis=0))
    one[...] = jnp.where(even, done[0], done[1])
    two[...] = jnp.where(even, done[1], done[0])


def load(b, d, face, u0, dx, u1, off, on, shift_out, stage, sems):
    where = place()
    nx, ny, _ = b.shape
    copies = [pltpu.make_async_copy(source, stage.at[k], sems.at[k]) for k, source in enumerate((b, d))]
    for copy in copies:
        copy.start()
    for k, (copy, into) in enumerate(zip(copies, (u0, dx))):
        copy.wait()

        def one(i, carry):
            main, rest = lanes(stage[k, i])
            into[0, i + 3, TOP : TOP + ny, :] = main
            into[1, i + 3, TOP : TOP + ny, :] = rest
            return carry

        lax.fori_loop(0, nx, one, 0, unroll=2)
    mid = ny // 2
    own = ny // 8
    for out, high in ((off, where[0]), (on, 1 - where[0])):
        for j in range(5):
            into, slab = (u0, 3 + j + high * (nx - 3)) if j < 3 else (dx, j + high * (nx - 2))
            at = j * (own + own // 2)
            out[at : at + own] = into[0, slab, TOP : TOP + ny, :].reshape(own, 8, 128)
            rest = into[1, slab, TOP : TOP + ny, :]
            out[at + own : at + own + own // 2] = (rest[:mid] + half_turn(rest[mid:])).reshape(own // 2, 8, 128)
    zero = jnp.zeros((8, 128), F32)
    inner = range(TOP + PART, TOP + ny - PART, PART)

    def probe(i, carry):
        norm, lift = carry
        at = 5 + 3 * i
        for row in inner:
            for p, new in enumerate(stencil(u0, dx, at, 6.0, row, PART)):
                mid = u0[p, at, row : row + PART, :]
                norm = norm + fold(mid * mid)
                lift = lift + fold(mid * new)
        return norm, lift

    norm, lift = lax.fori_loop(0, 4, probe, (zero, zero), unroll=2)
    norm = total(norm)
    lift = total(lift)
    shift = jnp.where(norm > 0.0, lift / jnp.where(norm > 0.0, norm, 1.0), SHIFT)
    shift = to_grain(jnp.clip(shift, 0.0, 14.0))
    shift_out[...] = shift
    base = 6.0 - shift[0:1, :]
    def first(i, carry):
        raised(u1, u0, dx, i, base, None, rows=inner)
        return carry

    lax.fori_loop(4, nx + 2, first, 0, unroll=2)


def lone(rest, second):
    rest = half_turn(rest) if second else rest
    return jnp.where(lax.broadcasted_iota(jnp.int32, rest.shape, rest.ndim - 1) < 64, rest, 0.0)


def corners(u0_in, dx_in, off_in, on_in, got_one, got_two, u0, dx, off, on):
    where = place()
    even = lax.axis_index("z") % 2 == 0
    nx = u0.shape[1] - 6
    ny = u0.shape[2] - 2 * TOP
    count = nx // 2 + nx // 4
    half = count // 2
    for side, row in enumerate((TOP - 8, TOP + ny)):
        first, second = (got_two, got_one) if side == 0 else (got_one, got_two)
        halo = jnp.where(even, first[...], second[...])
        rest = halo[count : count + half]
        for plane, tiles in enumerate((halo[:count], jnp.concatenate([lone(rest, False), lone(rest, True)], axis=0))):
            field = tiles[: nx // 2]
            shift = tiles[nx // 2 :]
            for k, turn in enumerate(FIELD_TURNS[side]):
                at = slice(3 + k * nx // 2, 3 + (k + 1) * nx // 2)
                u0[plane, at, row : row + 8, :] = pltpu.roll(field, 8 - turn, 1) if turn else field
            for k, turn in enumerate(SHIFT_TURNS):
                at = slice(3 + k * nx // 4, 3 + (k + 1) * nx // 4)
                dx[plane, at, row : row + 8, :] = pltpu.roll(shift, 8 - turn, 1) if turn else shift
    start = 5 * (ny // 8 + ny // 16)
    for out, high in ((off, where[0]), (on, 1 - where[0])):
        one = 3 + high * (nx - 1)
        two = 4 + high * (nx - 3)
        rests = []
        for j, (field, at) in enumerate(((u0, one), (u0, two), (dx, one))):
            tiles = []
            for plane in range(2):
                low = field[plane, at, TOP - 8 : TOP, :]
                tiles.append(jnp.where(iota(low.shape, 0) >= 4, low, field[plane, at, TOP + ny : TOP + ny + 8, :]))
            out[start + j] = tiles[0]
            rests.append(tiles[1])
        out[start + 3] = squeeze(rests[0], rests[1])
        out[start + 4] = rests[2]


def stencil(field, dx, at, base, row, rows):
    here = slice(row, row + rows)
    above = slice(row - 1, row + rows - 1)
    below = slice(row + 1, row + rows + 1)
    lane = iota((rows, 128), 1)
    mid = [field[p, at, here, :] for p in range(2)]
    beside = [
        (field[p, at - 1, here, :] + field[p, at + 1, here, :]) + (field[p, at, above, :] + field[p, at, below, :])
        for p in range(2)
    ]
    right = [pltpu.roll(a, 1, 1) for a in mid]
    left = [pltpu.roll(a, 127, 1) for a in mid]
    across = (
        jnp.where(lane == 0, right[1], right[0]) + jnp.where(lane == 127, left[1], left[0]),
        jnp.where(lane == 0, right[0], right[1]) + left[1],
    )
    new = [(dx[p, at, here, :] + base) * mid[p] - (beside[p] + across[p]) for p in range(2)]
    return new[0], jnp.where(lane < 64, new[1], 0.0)


def fold(a):
    return jnp.sum(a.reshape(-1, 8, 128), axis=0)


def total(a):
    return jnp.broadcast_to(jnp.sum(a, axis=(0, 1), keepdims=True), (8, 128))


def raised(into, field, dx, at, base, there, factor=None, rows=None):
    ny = field.shape[2] - 2 * TOP
    for row in rows or range(TOP, TOP + ny, PART):
        for p, new in enumerate(stencil(field, dx, at, base, row, PART)):
            into[p, at, row : row + PART, :] = new if factor is None else new * factor
    if there is None:
        return
    for row, edge in ((TOP - 8, there[0]), (TOP + ny, there[1])):
        edge = edge if factor is None else edge * factor
        for p, new in enumerate(stencil(field, dx, at, base, row, 8)):
            into[p, at, row : row + 8, :] = new * edge


def summed(u0, dx, u1, u2, u3, at, base, sums):
    ny = u0.shape[2] - 2 * TOP
    sums = list(sums)
    for row in range(TOP, TOP + ny, PART):
        here = slice(row, row + PART)
        for p, f3 in enumerate(stencil(u2, dx, at, base, row, PART)):
            u3[p, at - 3, row - TOP : row - TOP + PART, :] = f3
            f0 = u0[p, at, here, :]
            f1 = u1[p, at, here, :]
            f2 = u2[p, at, here, :]
            for k, product in enumerate((f0 * f0, f0 * f1, f1 * f1, f1 * f2, f2 * f2, f2 * f3)):
                sums[k] = sums[k] + fold(product)
    return tuple(sums)


def middle(u0, dx, u1_in, shift, u1, u2, u3, sums_out):
    where = place()
    nx = u0.shape[1] - 6
    ny = u0.shape[2] - 2 * TOP
    there = [where[k].astype(F32) for k in (3, 4)]
    zero = jnp.zeros((8, 128), F32)
    base = 6.0 - shift[0:1, :]

    def first(i, carry):
        raised(u1, u0, dx, i, base, there, rows=(TOP, TOP + ny - PART))
        return carry

    def second(i, carry):
        raised(u2, u1, dx, i, base, there)
        return carry

    def third(i, sums):
        return summed(u0, dx, u1, u2, u3, i, base, sums)

    lax.fori_loop(4, nx + 2, first, 0, unroll=2)
    lax.fori_loop(5, nx + 1, second, 0, unroll=2)
    sums = lax.fori_loop(6, nx, third, (zero,) * 6)
    for k in range(6):
        sums_out[k] = sums[k]


def rim(u0_in, dx_in, u1_in, u2_in, u3_in, sums_in, shift_in, off, on, u0, dx, u1, u2, u3, row_out):
    where = place()
    nx = u0.shape[1] - 6
    ny = u0.shape[2] - 2 * TOP
    there = [where[k].astype(F32) for k in (3, 4)]
    mid = ny // 2
    own = ny // 8
    start = 5 * (own + own // 2)
    for face, high in ((off, where[0]), (on, 1 - where[0])):
        for j in range(5):
            begin = j * (own + own // 2)
            rest = face[begin + own : begin + own + own // 2].reshape(mid, 128)
            field, at = (u0, j + high * (nx + 3)) if j < 3 else (dx, j - 2 + high * (nx + 2))
            field[0, at, TOP : TOP + ny, :] = face[begin : begin + own].reshape(ny, 128)
            field[1, at, TOP : TOP + mid, :] = lone(rest, False)
            field[1, at, TOP + mid : TOP + ny, :] = lone(rest, True)
        one = 2 + high * (nx + 1)
        two = 1 + high * (nx + 3)
        for j, (field, at) in enumerate(((u0, one), (u0, two), (dx, one))):
            for plane, tile in enumerate((face[start + j], lone(face[start + 3 + j // 2], j == 1))):
                field[plane, at, TOP - 8 : TOP, :] = tile
                field[plane, at, TOP + ny : TOP + ny + 8, :] = tile
    shift = shift_in[...]
    base = 6.0 - shift[0:1, :]
    low = where[1].astype(F32)
    high = where[2].astype(F32)

    def first(i, carry):
        raised(u1, u0, dx, 1 + i, base, there, jnp.where(i < 2, low, 1.0))
        raised(u1, u0, dx, nx + 2 + i, base, there, jnp.where(i > 0, high, 1.0))
        return carry

    def second(i, carry):
        raised(u2, u1, dx, 2 + i, base, there, jnp.where(i < 1, low, 1.0))
        raised(u2, u1, dx, nx + 1 + i, base, there, jnp.where(i > 1, high, 1.0))
        return carry

    def third(i, sums):
        for at in (3 + i, nx + i):
            sums = summed(u0, dx, u1, u2, u3, at, base, sums)
        return sums

    lax.fori_loop(0, 3, first, 0)
    lax.fori_loop(0, 3, second, 0)
    sums = lax.fori_loop(0, 3, third, tuple(sums_in[k] for k in range(6)))
    pairs = translated([(total(a), jnp.zeros((8, 128), F32)) for a in sums], shift - SHIFT)
    lane = iota((8, 128), 1)
    line = jnp.zeros((8, 128), F32)
    for k, (high_part, low_part) in enumerate(pairs):
        line = jnp.where(lane == k, high_part, jnp.where(lane == k + 6, low_part, line))
    for k in range(row_out.shape[0] // 8):
        row_out[8 * k : 8 * k + 8, :] = line


def gathered(rows):
    parts = [(rows[8 * k : 8 * k + 8], jnp.zeros((8, 128), F32)) for k in range(rows.shape[0] // 8)]

    def joined(one, two):
        s, e = two_sum(one[0], two[0])
        return s, e + (one[1] + two[1])

    while len(parts) > 1:
        parts = [joined(*parts[k : k + 2]) if k + 1 < len(parts) else parts[k] for k in range(0, len(parts), 2)]
    s, e = parts[0]
    for by in (4, 2, 1):
        s, e = joined((s, e), (pltpu.roll(s, by, 0), pltpu.roll(e, by, 0)))
    lane = iota((8, 128), 1)
    return jnp.where(lane < 6, s, s + pltpu.roll(e, 6, 1))


def regroup(rows, out):
    line = gathered(rows)
    for k in range(out.shape[0] // 8):
        out[8 * k : 8 * k + 8, :] = line


def steps_of(moments, centre):
    def form(one, two):
        out = 0.0
        for k in range(len(one) + len(two) - 1):
            part = 0.0
            for i in range(len(one)):
                if 0 <= k - i < len(two):
                    part = part + one[i] * two[k - i]
            out = out + part * moments[k]
        return out

    def plus(one, factor, two):
        size = max(len(one), len(two))
        out = []
        for k in range(size):
            if k >= len(two):
                out.append(one[k])
            elif k >= len(one):
                out.append(factor * two[k])
            else:
                out.append(one[k] + factor * two[k])
        return out

    unit = jnp.ones_like(moments[0])
    residual = [unit]
    solution_field = []
    s = []
    p = []
    for step in range(3):
        raised = [residual[0] * centre]
        for k in range(1, len(residual)):
            raised.append(residual[k - 1] + centre * residual[k])
        raised.append(residual[-1])
        gamma = form(residual, residual)
        delta = form(residual, raised)
        if step == 0:
            alpha = gamma / delta
            s, p = raised, residual
        else:
            beta = gamma / gamma_prev
            alpha = gamma / (delta - beta * gamma / alpha_prev)
            s = plus(raised, beta, s)
            p = plus(residual, beta, p)
        solution_field = plus(solution_field, alpha, p)
        residual = plus(residual, -alpha, s)
        gamma_prev = gamma
        alpha_prev = alpha
    return solution_field, residual


def recentred(coefficients, step):
    out = list(coefficients)
    size = len(out)
    for i in range(size - 1):
        for k in range(size - 2, i - 1, -1):
            out[k] = out[k] + step * out[k + 1]
    return out


def finish(rows, shift_in, u0, u1, u2, u3, solution_field, residual, xs_out, rs_out, sems):
    nx, ny, nz = xs_out.shape
    line = gathered(rows)

    def lane(k):
        one = jnp.where(iota((8, 128), 1) == k, line, 0.0)
        return jnp.broadcast_to(jnp.sum(one, axis=1, keepdims=True), (8, 128))

    moments = [(lane(k), lane(k + 6)) for k in range(6)]
    away = to_grain(moments[1][0] / moments[0][0])
    moments = [high + low for high, low in translated(moments, -away)]
    centre = SHIFT + away
    xs, rs = steps_of(moments, centre)
    step = shift_in[...] - centre
    xs = [a[0:1, :] for a in recentred(xs, step)]
    rs = [a[0:1, :] for a in recentred(rs, step)]
    part = nx // PARTS
    copies = []
    for k in range(PARTS):

        def one(i, carry):
            for p, (begin, width) in enumerate(((0, 128), (128, nz - 128))):
                own = pl.ds(TOP, ny)
                f = (u0[p, i + 3, own, :], u1[p, i + 3, own, :], u2[p, i + 3, own, :], u3[p, i])
                x = (xs[0] * f[0] + xs[1] * f[1]) + xs[2] * f[2]
                r = (rs[0] * f[0] + rs[1] * f[1]) + (rs[2] * f[2] + rs[3] * f[3])
                xs_out[i, :, begin : begin + width] = x[:, :width]
                rs_out[i, :, begin : begin + width] = r[:, :width]
            return carry

        lax.fori_loop(k * part, (k + 1) * part, one, 0)
        piece = pl.ds(k * part, part)
        for j, (source, target) in enumerate(((xs_out, solution_field), (rs_out, residual))):
            copy = pltpu.make_async_copy(source.at[piece], target.at[piece], sems.at[2 * k + j])
            copy.start()
            copies.append(copy)
    for copy in copies:
        copy.wait()


def swapped(a, axis, first):
    count = lax.axis_size(axis)
    pairs = []
    for k in range(first, count - 1, 2):
        pairs += [(k, k + 1), (k + 1, k)]
    return lax.ppermute(a, axis, pairs)


def spread(rows, axes):
    count = lax.axis_size(axes)
    out = lax.all_to_all(rows[:count].reshape(count, 1, 128), axes, 0, 0, tiled=True)
    return jnp.pad(out.reshape(count, 128), ((0, -count % 8), (0, 0)))


IN_VMEM = pl.BlockSpec(memory_space=pltpu.VMEM)
IN_HBM = pl.BlockSpec(memory_space=pltpu.HBM)


def call(body, name, outs, ins, scratch=(), aliases=None, out_specs=None, flops=0):
    return pl.pallas_call(
        body,
        out_shape=outs,
        in_specs=ins,
        out_specs=out_specs or (IN_VMEM,) * len(outs),
        scratch_shapes=list(scratch),
        input_output_aliases=aliases or {},
        compiler_params=pltpu.CompilerParams(vmem_limit_bytes=GRANT),
        cost_estimate=pl.CostEstimate(flops=flops, bytes_accessed=0, transcendentals=0) if flops else None,
        name=name,
    )


def on_device(right_side, diagonal):
    nx, ny, nz = right_side.shape
    rows = ny + 2 * TOP
    shape = lambda *dims: pltpu.VMEM(dims, F32)
    field = shape(2, nx + 6, rows, 128)
    y_face = shape((nx // 2 + nx // 4) * 3 // 2, 8, 128)
    x_face = shape(5 * (ny // 8 + ny // 16) + 5, 8, 128)
    right_side, diagonal = (pltpu.with_memory_space_constraint(a, pltpu.HBM) for a in (right_side, diagonal))
    y_one, y_two = call(
        pack_y,
        "pack_y",
        (y_face, y_face),
        (IN_HBM, IN_HBM),
        scratch=(pltpu.VMEM((4, nx, 8, nz), F32), pltpu.SemaphoreType.DMA((4,))),
    )(right_side, diagonal)
    got_one = swapped(y_one, "z", 0)
    got_two = swapped(y_two, "z", 1)
    u0, dx, u1, off, on, shift = call(
        load,
        "load",
        (field, field, field, x_face, x_face, shape(8, 128)),
        (IN_HBM, IN_HBM, IN_VMEM),
        scratch=(pltpu.VMEM((2, nx, ny, nz), F32), pltpu.SemaphoreType.DMA((2,))),
        flops=10_000_000,
    )(right_side, diagonal, y_one)
    u0, dx, off, on = call(
        corners,
        "corners",
        (field, field, x_face, x_face),
        (IN_VMEM,) * 6,
        aliases={k: k for k in range(4)},
    )(u0, dx, off, on, got_one, got_two)
    off = swapped(off, GX, 1)
    on = swapped(on, GX, 0)
    u1, u2, u3, sums = call(
        middle,
        "middle",
        (field, field, shape(2, nx, ny, 128), shape(6, 8, 128)),
        (IN_VMEM,) * 4,
        aliases={2: 0},
        flops=20_000_000,
    )(u0, dx, u1, shift)
    up = lambda n: -(-n // 8) * 8
    one = lax.axis_size(FIRST)
    two = lax.axis_size(SECOND)
    u0, dx, u1, u2, u3, line = call(
        rim,
        "rim",
        (field, field, field, field, shape(2, nx, ny, 128), shape(up(one), 128)),
        (IN_VMEM,) * 9,
        aliases={k: k for k in range(5)},
    )(u0, dx, u1, u2, u3, sums, shift, off, on)
    line = spread(line, FIRST)
    (line,) = call(regroup, "regroup", (shape(up(two), 128),), (IN_VMEM,))(line)
    line = spread(line, SECOND)
    whole = jax.ShapeDtypeStruct((nx, ny, nz), F32)
    return call(
        finish,
        "finish",
        (whole, whole),
        (IN_VMEM,) * 6,
        scratch=(pltpu.VMEM((nx, ny, nz), F32),) * 2 + (pltpu.SemaphoreType.DMA((2 * PARTS,)),),
        out_specs=(IN_HBM,) * 2,
    )(line, shift, u0, u1, u2, u3)


def solution_on(mesh, split):
    torus = Mesh(mesh.devices.reshape(*split, mesh.shape["gy"]), GX + ("z",))
    placed = (P(GX, "z", None), P(GX, "z", None))
    return jax.shard_map(on_device, mesh=torus, in_specs=placed, out_specs=placed, check_vma=False)


def solution(mesh):
    return solution_on(mesh, (8, 4, 2))
```

```python
import jax
import jax.numpy as jnp
from jax import lax
from jax.experimental import pallas as pl
from jax.experimental.pallas import tpu as pltpu
from jax.sharding import Mesh
from jax.sharding import PartitionSpec as P


SHIFT = 7.0
GRAIN = 8.0
GX = ("y", "x", "c")
FIRST = ("c", "z")
SECOND = ("y", "x")
F32 = jnp.float32
GRANT = 24 << 20
PARTS = 4
PART = 8
TOP = 16


def two_sum(a, b):
    s = a + b
    t = s - a
    return s, (a - (s - t)) + (b - t)


def halves(a):
    t = a * 4097.0
    high = t - (t - a)
    return high, a - high


def scaled(pair, factor):
    high, low = halves(pair[0])
    s, e = two_sum(high * factor, low * factor)
    return s, e + pair[1] * factor


def added(one, two):
    s, e = two_sum(one[0], two[0])
    return two_sum(s, e + (one[1] + two[1]))


def translated(moments, step):
    row = list(moments)
    out = [row[0]]
    while len(row) > 1:
        row = [added(row[k + 1], scaled(row[k], step)) for k in range(len(row) - 1)]
        out.append(row[0])
    return out


def to_grain(x):
    return jnp.floor(x * GRAIN + 0.5) / GRAIN


def iota(shape, dim):
    return lax.broadcasted_iota(jnp.int32, shape, dim)


def place():
    gx = lax.axis_index(GX)
    gy = lax.axis_index("z")
    is_there = lambda x: x.astype(jnp.int32)
    return (
        lax.axis_index("c"),
        is_there(gx > 0),
        is_there(gx < lax.axis_size(GX) - 1),
        is_there(gy > 0),
        is_there(gy < lax.axis_size("z") - 1),
    )


def half_turn(a):
    return pltpu.roll(a, 64, a.ndim - 1)


def squeeze(first, second):
    left = lax.broadcasted_iota(jnp.int32, first.shape, first.ndim - 1) < 64
    return jnp.where(left, first, half_turn(second))


def lanes(block):
    rest = jnp.pad(block[..., 128:], ((0, 0),) * (block.ndim - 1) + ((0, 64),))
    return block[..., :128], rest


def merged(tiles, turns, first_row):
    sub = iota(tiles[0].shape, 1)
    width = 8 // len(turns) if len(turns) > 2 else 3
    out = tiles[0]
    for k in range(1, len(turns)):
        here = pltpu.roll(tiles[k], turns[k], 1)
        start = (k * width) if first_row else (8 - width + turns[k]) % 8
        out = jnp.where((sub >= start) & (sub < start + width), here, out)
    return out


FIELD_TURNS = ((0, 5), (0, 3))
SHIFT_TURNS = (0, 2, 4, 6)


def pack_y(b, d, one, two, faces, sems):
    even = lax.axis_index("z") % 2 == 0
    nx, ny, _ = b.shape
    copies = [
        pltpu.make_async_copy(source.at[:, row : row + 8, :], faces.at[k], sems.at[k])
        for k, (source, row) in enumerate(((b, ny - 8), (d, ny - 8), (b, 0), (d, 0)))
    ]
    for copy in copies:
        copy.start()
    for copy in copies:
        copy.wait()
    done = []
    for side in range(2):
        field = faces[2 * side]
        shift = faces[2 * side + 1]
        field = merged([field[k * nx // 2 : (k + 1) * nx // 2] for k in range(2)], FIELD_TURNS[side], side == 1)
        shift = merged([shift[k * nx // 4 : (k + 1) * nx // 4] for k in range(4)], SHIFT_TURNS, side == 1)
        main, rest = lanes(jnp.concatenate([field, shift], axis=0))
        count = main.shape[0]
        done.append(jnp.concatenate([main, squeeze(rest[: count // 2], rest[count // 2 :])], axis=0))
    one[...] = jnp.where(even, done[0], done[1])
    two[...] = jnp.where(even, done[1], done[0])


def load(b, d, face, u0, dx, u1, off, on, shift_out, stage, sems):
    where = place()
    nx, ny, _ = b.shape
    copies = [pltpu.make_async_copy(source, stage.at[k], sems.at[k]) for k, source in enumerate((b, d))]
    for copy in copies:
        copy.start()
    for k, (copy, into) in enumerate(zip(copies, (u0, dx))):
        copy.wait()

        def one(i, carry):
            main, rest = lanes(stage[k, i])
            into[0, i + 3, TOP : TOP + ny, :] = main
            into[1, i + 3, TOP : TOP + ny, :] = rest
            return carry

        lax.fori_loop(0, nx, one, 0, unroll=2)
    mid = ny // 2
    own = ny // 8
    for out, high in ((off, where[0]), (on, 1 - where[0])):
        for j in range(5):
            into, slab = (u0, 3 + j + high * (nx - 3)) if j < 3 else (dx, j + high * (nx - 2))
            at = j * (own + own // 2)
            out[at : at + own] = into[0, slab, TOP : TOP + ny, :].reshape(own, 8, 128)
            rest = into[1, slab, TOP : TOP + ny, :]
            out[at + own : at + own + own // 2] = (rest[:mid] + half_turn(rest[mid:])).reshape(own // 2, 8, 128)
    zero = jnp.zeros((8, 128), F32)
    inner = range(TOP + PART, TOP + ny - PART, PART)

    def probe(i, carry):
        norm, lift = carry
        at = 5 + 3 * i
        for row in inner:
            for p, new in enumerate(stencil(u0, dx, at, 6.0, row, PART)):
                mid = u0[p, at, row : row + PART, :]
                norm = norm + fold(mid * mid)
                lift = lift + fold(mid * new)
        return norm, lift

    norm, lift = lax.fori_loop(0, 4, probe, (zero, zero), unroll=2)
    norm = total(norm)
    lift = total(lift)
    shift = jnp.where(norm > 0.0, lift / jnp.where(norm > 0.0, norm, 1.0), SHIFT)
    shift = to_grain(jnp.clip(shift, 0.0, 14.0))
    shift_out[...] = shift
    base = 6.0 - shift[0:1, :]
    def first(i, carry):
        raised(u1, u0, dx, i, base, None, rows=inner)
        return carry

    lax.fori_loop(4, nx + 2, first, 0, unroll=2)


def lone(rest, second):
    rest = half_turn(rest) if second else rest
    return jnp.where(lax.broadcasted_iota(jnp.int32, rest.shape, rest.ndim - 1) < 64, rest, 0.0)


def corners(u0_in, dx_in, off_in, on_in, got_one, got_two, u0, dx, off, on):
    where = place()
    even = lax.axis_index("z") % 2 == 0
    nx = u0.shape[1] - 6
    ny = u0.shape[2] - 2 * TOP
    count = nx // 2 + nx // 4
    half = count // 2
    for side, row in enumerate((TOP - 8, TOP + ny)):
        first, second = (got_two, got_one) if side == 0 else (got_one, got_two)
        halo = jnp.where(even, first[...], second[...])
        rest = halo[count : count + half]
        for plane, tiles in enumerate((halo[:count], jnp.concatenate([lone(rest, False), lone(rest, True)], axis=0))):
            field = tiles[: nx // 2]
            shift = tiles[nx // 2 :]
            for k, turn in enumerate(FIELD_TURNS[side]):
                at = slice(3 + k * nx // 2, 3 + (k + 1) * nx // 2)
                u0[plane, at, row : row + 8, :] = pltpu.roll(field, 8 - turn, 1) if turn else field
            for k, turn in enumerate(SHIFT_TURNS):
                at = slice(3 + k * nx // 4, 3 + (k + 1) * nx // 4)
                dx[plane, at, row : row + 8, :] = pltpu.roll(shift, 8 - turn, 1) if turn else shift
    start = 5 * (ny // 8 + ny // 16)
    for out, high in ((off, where[0]), (on, 1 - where[0])):
        one = 3 + high * (nx - 1)
        two = 4 + high * (nx - 3)
        rests = []
        for j, (field, at) in enumerate(((u0, one), (u0, two), (dx, one))):
            tiles = []
            for plane in range(2):
                low = field[plane, at, TOP - 8 : TOP, :]
                tiles.append(jnp.where(iota(low.shape, 0) >= 4, low, field[plane, at, TOP + ny : TOP + ny + 8, :]))
            out[start + j] = tiles[0]
            rests.append(tiles[1])
        out[start + 3] = squeeze(rests[0], rests[1])
        out[start + 4] = rests[2]


def stencil(field, dx, at, base, row, rows):
    here = slice(row, row + rows)
    above = slice(row - 1, row + rows - 1)
    below = slice(row + 1, row + rows + 1)
    lane = iota((rows, 128), 1)
    mid = [field[p, at, here, :] for p in range(2)]
    beside = [
        (field[p, at - 1, here, :] + field[p, at + 1, here, :]) + (field[p, at, above, :] + field[p, at, below, :])
        for p in range(2)
    ]
    right = [pltpu.roll(a, 1, 1) for a in mid]
    left = [pltpu.roll(a, 127, 1) for a in mid]
    across = (
        jnp.where(lane == 0, right[1], right[0]) + jnp.where(lane == 127, left[1], left[0]),
        jnp.where(lane == 0, right[0], right[1]) + left[1],
    )
    new = [(dx[p, at, here, :] + base) * mid[p] - (beside[p] + across[p]) for p in range(2)]
    return new[0], jnp.where(lane < 64, new[1], 0.0)


def fold(a):
    return jnp.sum(a.reshape(-1, 8, 128), axis=0)


def total(a):
    return jnp.broadcast_to(jnp.sum(a, axis=(0, 1), keepdims=True), (8, 128))


def raised(into, field, dx, at, base, there, factor=None, rows=None):
    ny = field.shape[2] - 2 * TOP
    for row in rows or range(TOP, TOP + ny, PART):
        for p, new in enumerate(stencil(field, dx, at, base, row, PART)):
            into[p, at, row : row + PART, :] = new if factor is None else new * factor
    if there is None:
        return
    for row, edge in ((TOP - 8, there[0]), (TOP + ny, there[1])):
        edge = edge if factor is None else edge * factor
        for p, new in enumerate(stencil(field, dx, at, base, row, 8)):
            into[p, at, row : row + 8, :] = new * edge


def summed(u0, dx, u1, u2, u3, at, base, sums):
    ny = u0.shape[2] - 2 * TOP
    sums = list(sums)
    for row in range(TOP, TOP + ny, PART):
        here = slice(row, row + PART)
        for p, f3 in enumerate(stencil(u2, dx, at, base, row, PART)):
            u3[p, at - 3, row - TOP : row - TOP + PART, :] = f3
            f0 = u0[p, at, here, :]
            f1 = u1[p, at, here, :]
            f2 = u2[p, at, here, :]
            for k, product in enumerate((f0 * f0, f0 * f1, f1 * f1, f1 * f2, f2 * f2, f2 * f3)):
                sums[k] = sums[k] + fold(product)
    return tuple(sums)


def middle(u0, dx, u1_in, shift, u1, u2, u3, sums_out):
    where = place()
    nx = u0.shape[1] - 6
    ny = u0.shape[2] - 2 * TOP
    there = [where[k].astype(F32) for k in (3, 4)]
    zero = jnp.zeros((8, 128), F32)
    base = 6.0 - shift[0:1, :]

    def first(i, carry):
        raised(u1, u0, dx, i, base, there, rows=(TOP, TOP + ny - PART))
        return carry

    def second(i, carry):
        raised(u2, u1, dx, i, base, there)
        return carry

    def third(i, sums):
        return summed(u0, dx, u1, u2, u3, i, base, sums)

    lax.fori_loop(4, nx + 2, first, 0, unroll=2)
    lax.fori_loop(5, nx + 1, second, 0, unroll=2)
    sums = lax.fori_loop(6, nx, third, (zero,) * 6)
    for k in range(6):
        sums_out[k] = sums[k]


def rim(u0_in, dx_in, u1_in, u2_in, u3_in, sums_in, shift_in, off, on, u0, dx, u1, u2, u3, row_out):
    where = place()
    nx = u0.shape[1] - 6
    ny = u0.shape[2] - 2 * TOP
    there = [where[k].astype(F32) for k in (3, 4)]
    mid = ny // 2
    own = ny // 8
    start = 5 * (own + own // 2)
    for face, high in ((off, where[0]), (on, 1 - where[0])):
        for j in range(5):
            begin = j * (own + own // 2)
            rest = face[begin + own : begin + own + own // 2].reshape(mid, 128)
            field, at = (u0, j + high * (nx + 3)) if j < 3 else (dx, j - 2 + high * (nx + 2))
            field[0, at, TOP : TOP + ny, :] = face[begin : begin + own].reshape(ny, 128)
            field[1, at, TOP : TOP + mid, :] = lone(rest, False)
            field[1, at, TOP + mid : TOP + ny, :] = lone(rest, True)
        one = 2 + high * (nx + 1)
        two = 1 + high * (nx + 3)
        for j, (field, at) in enumerate(((u0, one), (u0, two), (dx, one))):
            for plane, tile in enumerate((face[start + j], lone(face[start + 3 + j // 2], j == 1))):
                field[plane, at, TOP - 8 : TOP, :] = tile
                field[plane, at, TOP + ny : TOP + ny + 8, :] = tile
    shift = shift_in[...]
    base = 6.0 - shift[0:1, :]
    low = where[1].astype(F32)
    high = where[2].astype(F32)

    def first(i, carry):
        raised(u1, u0, dx, 1 + i, base, there, jnp.where(i < 2, low, 1.0))
        raised(u1, u0, dx, nx + 2 + i, base, there, jnp.where(i > 0, high, 1.0))
        return carry

    def second(i, carry):
        raised(u2, u1, dx, 2 + i, base, there, jnp.where(i < 1, low, 1.0))
        raised(u2, u1, dx, nx + 1 + i, base, there, jnp.where(i > 1, high, 1.0))
        return carry

    def third(i, sums):
        for at in (3 + i, nx + i):
            sums = summed(u0, dx, u1, u2, u3, at, base, sums)
        return sums

    lax.fori_loop(0, 3, first, 0)
    lax.fori_loop(0, 3, second, 0)
    sums = lax.fori_loop(0, 3, third, tuple(sums_in[k] for k in range(6)))
    pairs = translated([(total(a), jnp.zeros((8, 128), F32)) for a in sums], shift - SHIFT)
    lane = iota((8, 128), 1)
    line = jnp.zeros((8, 128), F32)
    for k, (high_part, low_part) in enumerate(pairs):
        line = jnp.where(lane == k, high_part, jnp.where(lane == k + 6, low_part, line))
    for k in range(row_out.shape[0] // 8):
        row_out[8 * k : 8 * k + 8, :] = line


def gathered(rows):
    parts = [(rows[8 * k : 8 * k + 8], jnp.zeros((8, 128), F32)) for k in range(rows.shape[0] // 8)]

    def joined(one, two):
        s, e = two_sum(one[0], two[0])
        return s, e + (one[1] + two[1])

    while len(parts) > 1:
        parts = [joined(*parts[k : k + 2]) if k + 1 < len(parts) else parts[k] for k in range(0, len(parts), 2)]
    s, e = parts[0]
    for by in (4, 2, 1):
        s, e = joined((s, e), (pltpu.roll(s, by, 0), pltpu.roll(e, by, 0)))
    lane = iota((8, 128), 1)
    return jnp.where(lane < 6, s, s + pltpu.roll(e, 6, 1))


def regroup(rows, out):
    line = gathered(rows)
    for k in range(out.shape[0] // 8):
        out[8 * k : 8 * k + 8, :] = line


def steps_of(moments, centre):
    def form(one, two):
        out = 0.0
        for k in range(len(one) + len(two) - 1):
            part = 0.0
            for i in range(len(one)):
                if 0 <= k - i < len(two):
                    part = part + one[i] * two[k - i]
            out = out + part * moments[k]
        return out

    def plus(one, factor, two):
        size = max(len(one), len(two))
        out = []
        for k in range(size):
            if k >= len(two):
                out.append(one[k])
            elif k >= len(one):
                out.append(factor * two[k])
            else:
                out.append(one[k] + factor * two[k])
        return out

    unit = jnp.ones_like(moments[0])
    residual = [unit]
    solution_field = []
    s = []
    p = []
    for step in range(3):
        raised = [residual[0] * centre]
        for k in range(1, len(residual)):
            raised.append(residual[k - 1] + centre * residual[k])
        raised.append(residual[-1])
        gamma = form(residual, residual)
        delta = form(residual, raised)
        if step == 0:
            alpha = gamma / delta
            s, p = raised, residual
        else:
            beta = gamma / gamma_prev
            alpha = gamma / (delta - beta * gamma / alpha_prev)
            s = plus(raised, beta, s)
            p = plus(residual, beta, p)
        solution_field = plus(solution_field, alpha, p)
        residual = plus(residual, -alpha, s)
        gamma_prev = gamma
        alpha_prev = alpha
    return solution_field, residual


def recentred(coefficients, step):
    out = list(coefficients)
    size = len(out)
    for i in range(size - 1):
        for k in range(size - 2, i - 1, -1):
            out[k] = out[k] + step * out[k + 1]
    return out


def finish(rows, shift_in, u0, u1, u2, u3, solution_field, residual, xs_out, rs_out, sems):
    nx, ny, nz = xs_out.shape
    line = gathered(rows)

    def lane(k):
        one = jnp.where(iota((8, 128), 1) == k, line, 0.0)
        return jnp.broadcast_to(jnp.sum(one, axis=1, keepdims=True), (8, 128))

    moments = [(lane(k), lane(k + 6)) for k in range(6)]
    away = to_grain(moments[1][0] / moments[0][0])
    moments = [high + low for high, low in translated(moments, -away)]
    centre = SHIFT + away
    xs, rs = steps_of(moments, centre)
    step = shift_in[...] - centre
    xs = [a[0:1, :] for a in recentred(xs, step)]
    rs = [a[0:1, :] for a in recentred(rs, step)]
    part = nx // PARTS
    copies = []
    for k in range(PARTS):

        def one(i, carry):
            for p, (begin, width) in enumerate(((0, 128), (128, nz - 128))):
                own = pl.ds(TOP, ny)
                f = (u0[p, i + 3, own, :], u1[p, i + 3, own, :], u2[p, i + 3, own, :], u3[p, i])
                x = (xs[0] * f[0] + xs[1] * f[1]) + xs[2] * f[2]
                r = (rs[0] * f[0] + rs[1] * f[1]) + (rs[2] * f[2] + rs[3] * f[3])
                xs_out[i, :, begin : begin + width] = x[:, :width]
                rs_out[i, :, begin : begin + width] = r[:, :width]
            return carry

        lax.fori_loop(k * part, (k + 1) * part, one, 0)
        piece = pl.ds(k * part, part)
        for j, (source, target) in enumerate(((xs_out, solution_field), (rs_out, residual))):
            copy = pltpu.make_async_copy(source.at[piece], target.at[piece], sems.at[2 * k + j])
            copy.start()
            copies.append(copy)
    for copy in copies:
        copy.wait()


def swapped(a, axis, first):
    count = lax.axis_size(axis)
    pairs = []
    for k in range(first, count - 1, 2):
        pairs += [(k, k + 1), (k + 1, k)]
    return lax.ppermute(a, axis, pairs)


def spread(rows, axes):
    count = lax.axis_size(axes)
    out = lax.all_to_all(rows[:count].reshape(count, 1, 128), axes, 0, 0, tiled=True)
    return jnp.pad(out.reshape(count, 128), ((0, -count % 8), (0, 0)))


IN_VMEM = pl.BlockSpec(memory_space=pltpu.VMEM)
IN_HBM = pl.BlockSpec(memory_space=pltpu.HBM)


def call(body, name, outs, ins, scratch=(), aliases=None, out_specs=None, flops=0):
    return pl.pallas_call(
        body,
        out_shape=outs,
        in_specs=ins,
        out_specs=out_specs or (IN_VMEM,) * len(outs),
        scratch_shapes=list(scratch),
        input_output_aliases=aliases or {},
        compiler_params=pltpu.CompilerParams(vmem_limit_bytes=GRANT),
        cost_estimate=pl.CostEstimate(flops=flops, bytes_accessed=0, transcendentals=0) if flops else None,
        name=name,
    )


def on_device(right_side, diagonal):
    nx, ny, nz = right_side.shape
    rows = ny + 2 * TOP
    shape = lambda *dims: pltpu.VMEM(dims, F32)
    field = shape(2, nx + 6, rows, 128)
    y_face = shape((nx // 2 + nx // 4) * 3 // 2, 8, 128)
    x_face = shape(5 * (ny // 8 + ny // 16) + 5, 8, 128)
    right_side, diagonal = (pltpu.with_memory_space_constraint(a, pltpu.HBM) for a in (right_side, diagonal))
    y_one, y_two = call(
        pack_y,
        "pack_y",
        (y_face, y_face),
        (IN_HBM, IN_HBM),
        scratch=(pltpu.VMEM((4, nx, 8, nz), F32), pltpu.SemaphoreType.DMA((4,))),
    )(right_side, diagonal)
    got_one = swapped(y_one, "z", 0)
    got_two = swapped(y_two, "z", 1)
    u0, dx, u1, off, on, shift = call(
        load,
        "load",
        (field, field, field, x_face, x_face, shape(8, 128)),
        (IN_HBM, IN_HBM, IN_VMEM),
        scratch=(pltpu.VMEM((2, nx, ny, nz), F32), pltpu.SemaphoreType.DMA((2,))),
        flops=10_000_000,
    )(right_side, diagonal, y_one)
    u0, dx, off, on = call(
        corners,
        "corners",
        (field, field, x_face, x_face),
        (IN_VMEM,) * 6,
        aliases={k: k for k in range(4)},
    )(u0, dx, off, on, got_one, got_two)
    off = swapped(off, GX, 1)
    on = swapped(on, GX, 0)
    u1, u2, u3, sums = call(
        middle,
        "middle",
        (field, field, shape(2, nx, ny, 128), shape(6, 8, 128)),
        (IN_VMEM,) * 4,
        aliases={2: 0},
        flops=20_000_000,
    )(u0, dx, u1, shift)
    up = lambda n: -(-n // 8) * 8
    one = lax.axis_size(FIRST)
    two = lax.axis_size(SECOND)
    u0, dx, u1, u2, u3, line = call(
        rim,
        "rim",
        (field, field, field, field, shape(2, nx, ny, 128), shape(up(one), 128)),
        (IN_VMEM,) * 9,
        aliases={k: k for k in range(5)},
    )(u0, dx, u1, u2, u3, sums, shift, off, on)
    line = spread(line, FIRST)
    (line,) = call(regroup, "regroup", (shape(up(two), 128),), (IN_VMEM,))(line)
    line = spread(line, SECOND)
    whole = jax.ShapeDtypeStruct((nx, ny, nz), F32)
    return call(
        finish,
        "finish",
        (whole, whole),
        (IN_VMEM,) * 6,
        scratch=(pltpu.VMEM((nx, ny, nz), F32),) * 2 + (pltpu.SemaphoreType.DMA((2 * PARTS,)),),
        out_specs=(IN_HBM,) * 2,
    )(line, shift, u0, u1, u2, u3)


def solution_on(mesh, split):
    torus = Mesh(mesh.devices.reshape(*split, mesh.shape["gy"]), GX + ("z",))
    placed = (P(GX, "z", None), P(GX, "z", None))
    return jax.shard_map(on_device, mesh=torus, in_specs=placed, out_specs=placed, check_vma=False)


def solution(mesh):
    return solution_on(mesh, (8, 4, 2))
```

```python
import jax
import jax.numpy as jnp
from jax import lax
from jax.experimental import pallas as pl
from jax.experimental.pallas import tpu as pltpu
from jax.sharding import Mesh
from jax.sharding import PartitionSpec as P


SHIFT = 7.0
GRAIN = 8.0
GX = ("y", "x", "c")
FIRST = ("c", "z")
SECOND = ("y", "x")
F32 = jnp.float32
GRANT = 24 << 20
PARTS = 4
PART = 16
TOP = 16


def two_sum(a, b):
    s = a + b
    t = s - a
    return s, (a - (s - t)) + (b - t)


def halves(a):
    t = a * 4097.0
    high = t - (t - a)
    return high, a - high


def scaled(pair, factor):
    high, low = halves(pair[0])
    s, e = two_sum(high * factor, low * factor)
    return s, e + pair[1] * factor


def added(one, two):
    s, e = two_sum(one[0], two[0])
    return two_sum(s, e + (one[1] + two[1]))


def translated(moments, step):
    row = list(moments)
    out = [row[0]]
    while len(row) > 1:
        row = [added(row[k + 1], scaled(row[k], step)) for k in range(len(row) - 1)]
        out.append(row[0])
    return out


def to_grain(x):
    return jnp.floor(x * GRAIN + 0.5) / GRAIN


def iota(shape, dim):
    return lax.broadcasted_iota(jnp.int32, shape, dim)


def place():
    gx = lax.axis_index(GX)
    gy = lax.axis_index("z")
    is_there = lambda x: x.astype(jnp.int32)
    return (
        lax.axis_index("c"),
        is_there(gx > 0),
        is_there(gx < lax.axis_size(GX) - 1),
        is_there(gy > 0),
        is_there(gy < lax.axis_size("z") - 1),
    )


def half_turn(a):
    return pltpu.roll(a, 64, a.ndim - 1)


def squeeze(first, second):
    left = lax.broadcasted_iota(jnp.int32, first.shape, first.ndim - 1) < 64
    return jnp.where(left, first, half_turn(second))


def lanes(block):
    rest = jnp.pad(block[..., 128:], ((0, 0),) * (block.ndim - 1) + ((0, 64),))
    return block[..., :128], rest


def merged(tiles, turns, first_row):
    sub = iota(tiles[0].shape, 1)
    width = 8 // len(turns) if len(turns) > 2 else 3
    out = tiles[0]
    for k in range(1, len(turns)):
        here = pltpu.roll(tiles[k], turns[k], 1)
        start = (k * width) if first_row else (8 - width + turns[k]) % 8
        out = jnp.where((sub >= start) & (sub < start + width), here, out)
    return out


FIELD_TURNS = ((0, 5), (0, 3))
SHIFT_TURNS = (0, 2, 4, 6)


def pack_y(b, d, one, two, faces, sems):
    even = lax.axis_index("z") % 2 == 0
    nx, ny, _ = b.shape
    copies = [
        pltpu.make_async_copy(source.at[:, row : row + 8, :], faces.at[k], sems.at[k])
        for k, (source, row) in enumerate(((b, ny - 8), (d, ny - 8), (b, 0), (d, 0)))
    ]
    for copy in copies:
        copy.start()
    for copy in copies:
        copy.wait()
    done = []
    for side in range(2):
        field = faces[2 * side]
        shift = faces[2 * side + 1]
        field = merged([field[k * nx // 2 : (k + 1) * nx // 2] for k in range(2)], FIELD_TURNS[side], side == 1)
        shift = merged([shift[k * nx // 4 : (k + 1) * nx // 4] for k in range(4)], SHIFT_TURNS, side == 1)
        main, rest = lanes(jnp.concatenate([field, shift], axis=0))
        count = main.shape[0]
        done.append(jnp.concatenate([main, squeeze(rest[: count // 2], rest[count // 2 :])], axis=0))
    one[...] = jnp.where(even, done[0], done[1])
    two[...] = jnp.where(even, done[1], done[0])


def load(b, d, face, u0, dx, u1, off, on, shift_out):
    where = place()
    nx, ny, _ = b.shape
    for source, into in ((b, u0), (d, dx)):

        def one(i, carry):
            main, rest = lanes(source[i])
            into[0, i + 3, TOP : TOP + ny, :] = main
            into[1, i + 3, TOP : TOP + ny, :] = rest
            return carry

        lax.fori_loop(0, nx, one, 0, unroll=2)
    mid = ny // 2
    own = ny // 8
    for out, high in ((off, where[0]), (on, 1 - where[0])):
        for j in range(5):
            into, slab = (u0, 3 + j + high * (nx - 3)) if j < 3 else (dx, j + high * (nx - 2))
            at = j * (own + own // 2)
            out[at : at + own] = into[0, slab, TOP : TOP + ny, :].reshape(own, 8, 128)
            rest = into[1, slab, TOP : TOP + ny, :]
            out[at + own : at + own + own // 2] = (rest[:mid] + half_turn(rest[mid:])).reshape(own // 2, 8, 128)
    zero = jnp.zeros((8, 128), F32)
    inner = range(TOP + PART, TOP + ny - PART, PART)

    def probe(i, carry):
        norm, lift = carry
        at = 5 + 3 * i
        for row in inner:
            for p, new in enumerate(stencil(u0, dx, at, 6.0, row, PART)):
                mid = u0[p, at, row : row + PART, :]
                norm = norm + fold(mid * mid)
                lift = lift + fold(mid * new)
        return norm, lift

    norm, lift = lax.fori_loop(0, 4, probe, (zero, zero), unroll=2)
    norm = total(norm)
    lift = total(lift)
    shift = jnp.where(norm > 0.0, lift / jnp.where(norm > 0.0, norm, 1.0), SHIFT)
    shift = to_grain(jnp.clip(shift, 0.0, 14.0))
    shift_out[...] = shift
    base = 6.0 - shift[0:1, :]
    def first(i, carry):
        raised(u1, u0, dx, i, base, None, rows=inner)
        return carry

    lax.fori_loop(4, nx + 2, first, 0, unroll=2)


def lone(rest, second):
    rest = half_turn(rest) if second else rest
    return jnp.where(lax.broadcasted_iota(jnp.int32, rest.shape, rest.ndim - 1) < 64, rest, 0.0)


def corners(u0_in, dx_in, off_in, on_in, got_one, got_two, u0, dx, off, on):
    where = place()
    even = lax.axis_index("z") % 2 == 0
    nx = u0.shape[1] - 6
    ny = u0.shape[2] - 2 * TOP
    count = nx // 2 + nx // 4
    half = count // 2
    for side, row in enumerate((TOP - 8, TOP + ny)):
        first, second = (got_two, got_one) if side == 0 else (got_one, got_two)
        halo = jnp.where(even, first[...], second[...])
        rest = halo[count : count + half]
        for plane, tiles in enumerate((halo[:count], jnp.concatenate([lone(rest, False), lone(rest, True)], axis=0))):
            field = tiles[: nx // 2]
            shift = tiles[nx // 2 :]
            for k, turn in enumerate(FIELD_TURNS[side]):
                at = slice(3 + k * nx // 2, 3 + (k + 1) * nx // 2)
                u0[plane, at, row : row + 8, :] = pltpu.roll(field, 8 - turn, 1) if turn else field
            for k, turn in enumerate(SHIFT_TURNS):
                at = slice(3 + k * nx // 4, 3 + (k + 1) * nx // 4)
                dx[plane, at, row : row + 8, :] = pltpu.roll(shift, 8 - turn, 1) if turn else shift
    start = 5 * (ny // 8 + ny // 16)
    for out, high in ((off, where[0]), (on, 1 - where[0])):
        one = 3 + high * (nx - 1)
        two = 4 + high * (nx - 3)
        rests = []
        for j, (field, at) in enumerate(((u0, one), (u0, two), (dx, one))):
            tiles = []
            for plane in range(2):
                low = field[plane, at, TOP - 8 : TOP, :]
                tiles.append(jnp.where(iota(low.shape, 0) >= 4, low, field[plane, at, TOP + ny : TOP + ny + 8, :]))
            out[start + j] = tiles[0]
            rests.append(tiles[1])
        out[start + 3] = squeeze(rests[0], rests[1])
        out[start + 4] = rests[2]


def stencil(field, dx, at, base, row, rows):
    here = slice(row, row + rows)
    above = slice(row - 1, row + rows - 1)
    below = slice(row + 1, row + rows + 1)
    lane = iota((rows, 128), 1)
    mid = [field[p, at, here, :] for p in range(2)]
    beside = [
        (field[p, at - 1, here, :] + field[p, at + 1, here, :]) + (field[p, at, above, :] + field[p, at, below, :])
        for p in range(2)
    ]
    right = [pltpu.roll(a, 1, 1) for a in mid]
    left = [pltpu.roll(a, 127, 1) for a in mid]
    across = (
        jnp.where(lane == 0, right[1], right[0]) + jnp.where(lane == 127, left[1], left[0]),
        jnp.where(lane == 0, right[0], right[1]) + left[1],
    )
    new = [(dx[p, at, here, :] + base) * mid[p] - (beside[p] + across[p]) for p in range(2)]
    return new[0], jnp.where(lane < 64, new[1], 0.0)


def fold(a):
    return jnp.sum(a.reshape(-1, 8, 128), axis=0)


def total(a):
    return jnp.broadcast_to(jnp.sum(a, axis=(0, 1), keepdims=True), (8, 128))


def raised(into, field, dx, at, base, there, factor=None, rows=None):
    ny = field.shape[2] - 2 * TOP
    for row in rows or range(TOP, TOP + ny, PART):
        for p, new in enumerate(stencil(field, dx, at, base, row, PART)):
            into[p, at, row : row + PART, :] = new if factor is None else new * factor
    if there is None:
        return
    for row, edge in ((TOP - 8, there[0]), (TOP + ny, there[1])):
        edge = edge if factor is None else edge * factor
        for p, new in enumerate(stencil(field, dx, at, base, row, 8)):
            into[p, at, row : row + 8, :] = new * edge


def summed(u0, dx, u1, u2, u3, at, base, sums):
    ny = u0.shape[2] - 2 * TOP
    sums = list(sums)
    for row in range(TOP, TOP + ny, PART):
        here = slice(row, row + PART)
        for p, f3 in enumerate(stencil(u2, dx, at, base, row, PART)):
            u3[p, at - 3, row - TOP : row - TOP + PART, :] = f3
            f0 = u0[p, at, here, :]
            f1 = u1[p, at, here, :]
            f2 = u2[p, at, here, :]
            for k, product in enumerate((f0 * f0, f0 * f1, f1 * f1, f1 * f2, f2 * f2, f2 * f3)):
                sums[k] = sums[k] + fold(product)
    return tuple(sums)


def middle(u0, dx, u1_in, shift, u1, u2, u3, sums_out):
    where = place()
    nx = u0.shape[1] - 6
    ny = u0.shape[2] - 2 * TOP
    there = [where[k].astype(F32) for k in (3, 4)]
    zero = jnp.zeros((8, 128), F32)
    base = 6.0 - shift[0:1, :]

    def first(i, carry):
        raised(u1, u0, dx, i, base, there, rows=(TOP, TOP + ny - PART))
        return carry

    def second(i, carry):
        raised(u2, u1, dx, i, base, there)
        return carry

    def third(i, sums):
        return summed(u0, dx, u1, u2, u3, i, base, sums)

    lax.fori_loop(4, nx + 2, first, 0, unroll=2)
    lax.fori_loop(5, nx + 1, second, 0, unroll=2)
    sums = lax.fori_loop(6, nx, third, (zero,) * 6)
    for k in range(6):
        sums_out[k] = sums[k]


def rim(u0_in, dx_in, u1_in, u2_in, u3_in, sums_in, shift_in, off, on, u0, dx, u1, u2, u3, row_out):
    where = place()
    nx = u0.shape[1] - 6
    ny = u0.shape[2] - 2 * TOP
    there = [where[k].astype(F32) for k in (3, 4)]
    mid = ny // 2
    own = ny // 8
    start = 5 * (own + own // 2)
    for face, high in ((off, where[0]), (on, 1 - where[0])):
        for j in range(5):
            begin = j * (own + own // 2)
            rest = face[begin + own : begin + own + own // 2].reshape(mid, 128)
            field, at = (u0, j + high * (nx + 3)) if j < 3 else (dx, j - 2 + high * (nx + 2))
            field[0, at, TOP : TOP + ny, :] = face[begin : begin + own].reshape(ny, 128)
            field[1, at, TOP : TOP + mid, :] = lone(rest, False)
            field[1, at, TOP + mid : TOP + ny, :] = lone(rest, True)
        one = 2 + high * (nx + 1)
        two = 1 + high * (nx + 3)
        for j, (field, at) in enumerate(((u0, one), (u0, two), (dx, one))):
            for plane, tile in enumerate((face[start + j], lone(face[start + 3 + j // 2], j == 1))):
                field[plane, at, TOP - 8 : TOP, :] = tile
                field[plane, at, TOP + ny : TOP + ny + 8, :] = tile
    shift = shift_in[...]
    base = 6.0 - shift[0:1, :]
    low = where[1].astype(F32)
    high = where[2].astype(F32)

    def first(i, carry):
        raised(u1, u0, dx, 1 + i, base, there, jnp.where(i < 2, low, 1.0))
        raised(u1, u0, dx, nx + 2 + i, base, there, jnp.where(i > 0, high, 1.0))
        return carry

    def second(i, carry):
        raised(u2, u1, dx, 2 + i, base, there, jnp.where(i < 1, low, 1.0))
        raised(u2, u1, dx, nx + 1 + i, base, there, jnp.where(i > 1, high, 1.0))
        return carry

    def third(i, sums):
        for at in (3 + i, nx + i):
            sums = summed(u0, dx, u1, u2, u3, at, base, sums)
        return sums

    lax.fori_loop(0, 3, first, 0)
    lax.fori_loop(0, 3, second, 0)
    sums = lax.fori_loop(0, 3, third, tuple(sums_in[k] for k in range(6)))
    pairs = translated([(total(a), jnp.zeros((8, 128), F32)) for a in sums], shift - SHIFT)
    lane = iota((8, 128), 1)
    line = jnp.zeros((8, 128), F32)
    for k, (high_part, low_part) in enumerate(pairs):
        line = jnp.where(lane == k, high_part, jnp.where(lane == k + 6, low_part, line))
    for k in range(row_out.shape[0] // 8):
        row_out[8 * k : 8 * k + 8, :] = line


def gathered(rows):
    parts = [(rows[8 * k : 8 * k + 8], jnp.zeros((8, 128), F32)) for k in range(rows.shape[0] // 8)]

    def joined(one, two):
        s, e = two_sum(one[0], two[0])
        return s, e + (one[1] + two[1])

    while len(parts) > 1:
        parts = [joined(*parts[k : k + 2]) if k + 1 < len(parts) else parts[k] for k in range(0, len(parts), 2)]
    s, e = parts[0]
    for by in (4, 2, 1):
        s, e = joined((s, e), (pltpu.roll(s, by, 0), pltpu.roll(e, by, 0)))
    lane = iota((8, 128), 1)
    return jnp.where(lane < 6, s, s + pltpu.roll(e, 6, 1))


def regroup(rows, out):
    line = gathered(rows)
    for k in range(out.shape[0] // 8):
        out[8 * k : 8 * k + 8, :] = line


def steps_of(moments, centre):
    def form(one, two):
        out = 0.0
        for k in range(len(one) + len(two) - 1):
            part = 0.0
            for i in range(len(one)):
                if 0 <= k - i < len(two):
                    part = part + one[i] * two[k - i]
            out = out + part * moments[k]
        return out

    def plus(one, factor, two):
        size = max(len(one), len(two))
        out = []
        for k in range(size):
            if k >= len(two):
                out.append(one[k])
            elif k >= len(one):
                out.append(factor * two[k])
            else:
                out.append(one[k] + factor * two[k])
        return out

    unit = jnp.ones_like(moments[0])
    residual = [unit]
    solution_field = []
    s = []
    p = []
    for step in range(3):
        raised = [residual[0] * centre]
        for k in range(1, len(residual)):
            raised.append(residual[k - 1] + centre * residual[k])
        raised.append(residual[-1])
        gamma = form(residual, residual)
        delta = form(residual, raised)
        if step == 0:
            alpha = gamma / delta
            s, p = raised, residual
        else:
            beta = gamma / gamma_prev
            alpha = gamma / (delta - beta * gamma / alpha_prev)
            s = plus(raised, beta, s)
            p = plus(residual, beta, p)
        solution_field = plus(solution_field, alpha, p)
        residual = plus(residual, -alpha, s)
        gamma_prev = gamma
        alpha_prev = alpha
    return solution_field, residual


def recentred(coefficients, step):
    out = list(coefficients)
    size = len(out)
    for i in range(size - 1):
        for k in range(size - 2, i - 1, -1):
            out[k] = out[k] + step * out[k + 1]
    return out


def finish(rows, shift_in, u0, u1, u2, u3, solution_field, residual, xs_out, rs_out, sems):
    nx, ny, nz = xs_out.shape
    line = gathered(rows)

    def lane(k):
        one = jnp.where(iota((8, 128), 1) == k, line, 0.0)
        return jnp.broadcast_to(jnp.sum(one, axis=1, keepdims=True), (8, 128))

    moments = [(lane(k), lane(k + 6)) for k in range(6)]
    away = to_grain(moments[1][0] / moments[0][0])
    moments = [high + low for high, low in translated(moments, -away)]
    centre = SHIFT + away
    xs, rs = steps_of(moments, centre)
    step = shift_in[...] - centre
    xs = [a[0:1, :] for a in recentred(xs, step)]
    rs = [a[0:1, :] for a in recentred(rs, step)]
    part = nx // PARTS
    copies = []
    for k in range(PARTS):

        def one(i, carry):
            for p, (begin, width) in enumerate(((0, 128), (128, nz - 128))):
                own = pl.ds(TOP, ny)
                f = (u0[p, i + 3, own, :], u1[p, i + 3, own, :], u2[p, i + 3, own, :], u3[p, i])
                x = (xs[0] * f[0] + xs[1] * f[1]) + xs[2] * f[2]
                r = (rs[0] * f[0] + rs[1] * f[1]) + (rs[2] * f[2] + rs[3] * f[3])
                xs_out[i, :, begin : begin + width] = x[:, :width]
                rs_out[i, :, begin : begin + width] = r[:, :width]
            return carry

        lax.fori_loop(k * part, (k + 1) * part, one, 0)
        piece = pl.ds(k * part, part)
        for j, (source, target) in enumerate(((xs_out, solution_field), (rs_out, residual))):
            copy = pltpu.make_async_copy(source.at[piece], target.at[piece], sems.at[2 * k + j])
            copy.start()
            copies.append(copy)
    for copy in copies:
        copy.wait()


def swapped(a, axis, first):
    count = lax.axis_size(axis)
    pairs = []
    for k in range(first, count - 1, 2):
        pairs += [(k, k + 1), (k + 1, k)]
    return lax.ppermute(a, axis, pairs)


def spread(rows, axes):
    count = lax.axis_size(axes)
    out = lax.all_to_all(rows[:count].reshape(count, 1, 128), axes, 0, 0, tiled=True)
    return jnp.pad(out.reshape(count, 128), ((0, -count % 8), (0, 0)))


IN_VMEM = pl.BlockSpec(memory_space=pltpu.VMEM)
IN_HBM = pl.BlockSpec(memory_space=pltpu.HBM)


def call(body, name, outs, ins, scratch=(), aliases=None, out_specs=None, flops=0):
    return pl.pallas_call(
        body,
        out_shape=outs,
        in_specs=ins,
        out_specs=out_specs or (IN_VMEM,) * len(outs),
        scratch_shapes=list(scratch),
        input_output_aliases=aliases or {},
        compiler_params=pltpu.CompilerParams(vmem_limit_bytes=GRANT),
        cost_estimate=pl.CostEstimate(flops=flops, bytes_accessed=0, transcendentals=0) if flops else None,
        name=name,
    )


def on_device(right_side, diagonal):
    nx, ny, nz = right_side.shape
    rows = ny + 2 * TOP
    shape = lambda *dims: pltpu.VMEM(dims, F32)
    field = shape(2, nx + 6, rows, 128)
    y_face = shape((nx // 2 + nx // 4) * 3 // 2, 8, 128)
    x_face = shape(5 * (ny // 8 + ny // 16) + 5, 8, 128)
    y_one, y_two = call(
        pack_y,
        "pack_y",
        (y_face, y_face),
        (IN_HBM, IN_HBM),
        scratch=(pltpu.VMEM((4, nx, 8, nz), F32), pltpu.SemaphoreType.DMA((4,))),
    )(*(pltpu.with_memory_space_constraint(a, pltpu.HBM) for a in (right_side, diagonal)))
    got_one = swapped(y_one, "z", 0)
    got_two = swapped(y_two, "z", 1)
    u0, dx, u1, off, on, shift = call(
        load,
        "load",
        (field, field, field, x_face, x_face, shape(8, 128)),
        (IN_VMEM,) * 3,
        flops=10_000_000,
    )(right_side, diagonal, y_one)
    u0, dx, off, on = call(
        corners,
        "corners",
        (field, field, x_face, x_face),
        (IN_VMEM,) * 6,
        aliases={k: k for k in range(4)},
    )(u0, dx, off, on, got_one, got_two)
    off = swapped(off, GX, 1)
    on = swapped(on, GX, 0)
    u1, u2, u3, sums = call(
        middle,
        "middle",
        (field, field, shape(2, nx, ny, 128), shape(6, 8, 128)),
        (IN_VMEM,) * 4,
        aliases={2: 0},
        flops=20_000_000,
    )(u0, dx, u1, shift)
    up = lambda n: -(-n // 8) * 8
    one = lax.axis_size(FIRST)
    two = lax.axis_size(SECOND)
    u0, dx, u1, u2, u3, line = call(
        rim,
        "rim",
        (field, field, field, field, shape(2, nx, ny, 128), shape(up(one), 128)),
        (IN_VMEM,) * 9,
        aliases={k: k for k in range(5)},
    )(u0, dx, u1, u2, u3, sums, shift, off, on)
    line = spread(line, FIRST)
    (line,) = call(regroup, "regroup", (shape(up(two), 128),), (IN_VMEM,))(line)
    line = spread(line, SECOND)
    whole = jax.ShapeDtypeStruct((nx, ny, nz), F32)
    return call(
        finish,
        "finish",
        (whole, whole),
        (IN_VMEM,) * 6,
        scratch=(pltpu.VMEM((nx, ny, nz), F32),) * 2 + (pltpu.SemaphoreType.DMA((2 * PARTS,)),),
        out_specs=(IN_HBM,) * 2,
    )(line, shift, u0, u1, u2, u3)


def solution_on(mesh, split):
    torus = Mesh(mesh.devices.reshape(*split, mesh.shape["gy"]), GX + ("z",))
    placed = (P(GX, "z", None), P(GX, "z", None))
    return jax.shard_map(on_device, mesh=torus, in_specs=placed, out_specs=placed, check_vma=False)


def solution(mesh):
    return solution_on(mesh, (8, 4, 2))
```
